128 devices in a mesh: gx: 16 (over z_hi, y, core), gy: 8 (over x, z_lo).
Axes of the slice: x: 4, y: 4, z: 4 (z_hi: 2, z_lo: 2; z = z_hi * 2 + z_lo), core: 2. Of those that a mesh axis runs over, the one named last changes fastest.
Arguments:
- tracer_amounts: bfloat16 [2, 1024, 1024, 128], P(None, ('gx', 'gy')), may hold values from 0.099609375 to 3
- zonal_transit_ratio: float32 [2, 1024, 1024], P(None, 'gx', 'gy'), may hold values from -0.5 to 0.5
- meridional_transit_ratio: float32 [2, 1024, 1024], P(None, 'gx', 'gy'), may hold values from -0.45 to 0.45
- moisture_ratio: float32 [2, 1024, 1024], P(None, 'gx', 'gy'), may hold values from 0.2 to 0.9
- stratum_depths: float32 [2, 1024, 1024], P(None, 'gx', 'gy'), may hold values from 0.5 to 2
- sun_elevation_factor: float32 [1024, 1024], P('gx', 'gy'), may hold values from 0.2 to 1
- thermal_anomaly: float32 [2, 1024, 1024], P(None, 'gx', 'gy'), may hold values from -6 to 6
- particle_class_map: int32 [1024, 1024], P(('gx', 'gy')), may hold values from 0 to 7
- ground_cover_kind: int32 [1024, 1024], P(('gx', 'gy')), may hold values from 0 to 23
- arid_extinction_table: bfloat16 [128, 64], replicated, may hold values from 0 to 0.015625
- swelling_factors: bfloat16 [128, 64], replicated, may hold values from 0 to 0.00390625
- settling_velocities: float32 [24, 128], replicated, may hold values from 0.05 to 2
- arriving_irradiance: float32 [4], replicated, may hold values from 0.5 to 2
Outputs:
- updated_tracer_amounts: float32 [2, 1024, 1024, 128], P(None, ('gx', 'gy'))
- updated_thermal_anomaly: float32 [2, 1024, 1024], P(None, 'gx', 'gy')
The draws below stay inside these ranges and needn't reach their ends.
All inputs are finite; a program needn't handle non-finite values.
Results may differ from the reference program's by a relative error of at most 0.00075.
Values may be sent and summed in bfloat16 or wider, within the bound.
No kernel may reach another device: no remote copies, remote signals or barrier semaphores. Data moves between devices by JAX's collectives and lax.ppermute only.
A program may use at most 128 MiB of HBM per device.

```python
import math
import jax
import jax.numpy as jnp
from jax import lax

S = 128
VERTICAL_TIERS = 2
SUB = 3
NBIN = 8
NW = 4
NLU = 24
ZONAL_POINTS = 1024
MERIDIONAL_NODES = 1024


def touch_ends(drawn, own_key, least, largest):
    place = [jax.random.randint(jax.random.fold_in(own_key, axis), (), 0, length) for axis, length in enumerate(drawn.shape)]
    main_axis = drawn.shape.index(max(drawn.shape))
    neighbour = place[:main_axis] + [(place[main_axis] + 1) % drawn.shape[main_axis]] + place[main_axis + 1:]
    return drawn.at[tuple(place)].set(least).at[tuple(neighbour)].set(largest)


def shard_levels(own_key, dims, split, least, largest):
    level = 1.0
    for dim, parts in split:
        steps = jax.random.uniform(jax.random.fold_in(jax.random.fold_in(own_key, 6), dim), (parts,), jnp.float32, least / len(split), largest / len(split))
        level = level * jnp.repeat(jnp.exp(steps), dims[dim] // parts).reshape((-1,) + (1,) * (len(dims) - 1 - dim))
    return level


def centred(own_key, shape, scale, most, cuts=(), held_as=jnp.bfloat16):
    loudness = shard_levels(own_key, shape, cuts, -0.22, 0.18) if cuts else 1.0
    entries = jax.random.normal(own_key, shape, jnp.float32) * scale * loudness
    return jnp.minimum(jnp.maximum(entries, -most), most).astype(held_as)


def setup_inputs(seed: int = 0) -> dict:
    streams_of = jax.random.split(jax.random.key(seed), 14)
    return {
        "tracer_amounts": jnp.clip(jnp.exp(math.log(3.0) - 3.4051113 * jax.random.uniform(streams_of[0], (VERTICAL_TIERS, ZONAL_POINTS, MERIDIONAL_NODES, S), jnp.float32) ** shard_levels(streams_of[0], (VERTICAL_TIERS, ZONAL_POINTS, MERIDIONAL_NODES, S), ((1, 128),), -0.2, 0.2)), 0.099609375, 3.0).astype(jnp.bfloat16),
        "zonal_transit_ratio": jnp.clip(jax.random.uniform(streams_of[1], (VERTICAL_TIERS, ZONAL_POINTS, MERIDIONAL_NODES), jnp.float32, -0.5, 0.5) * shard_levels(streams_of[1], (VERTICAL_TIERS, ZONAL_POINTS, MERIDIONAL_NODES), ((1, 16), (2, 8)), -0.4, 0.0), -0.5, 0.5),
        "meridional_transit_ratio": jnp.clip(jax.random.uniform(streams_of[2], (VERTICAL_TIERS, ZONAL_POINTS, MERIDIONAL_NODES), jnp.float32, -0.45, 0.45) * shard_levels(streams_of[2], (VERTICAL_TIERS, ZONAL_POINTS, MERIDIONAL_NODES), ((1, 16), (2, 8)), -0.4, 0.0), -0.45, 0.45),
        "moisture_ratio": jnp.clip(0.2 + 0.7 * jax.random.uniform(streams_of[3], (VERTICAL_TIERS, ZONAL_POINTS, MERIDIONAL_NODES), jnp.float32) ** shard_levels(streams_of[3], (VERTICAL_TIERS, ZONAL_POINTS, MERIDIONAL_NODES), ((1, 16), (2, 8)), -0.2, 0.2), 0.2, 0.9),
        "stratum_depths": jnp.clip(jnp.exp(math.log(2.0) - 1.3862944 * jax.random.uniform(streams_of[4], (VERTICAL_TIERS, ZONAL_POINTS, MERIDIONAL_NODES), jnp.float32) ** shard_levels(streams_of[4], (VERTICAL_TIERS, ZONAL_POINTS, MERIDIONAL_NODES), ((1, 16), (2, 8)), -0.2, 0.2)), 0.5, 2.0),
        "sun_elevation_factor": jnp.clip(jnp.exp(math.log(1.0) - 1.609438 * jax.random.uniform(streams_of[5], (ZONAL_POINTS, MERIDIONAL_NODES), jnp.float32) ** shard_levels(streams_of[5], (ZONAL_POINTS, MERIDIONAL_NODES), ((0, 16), (1, 8)), -0.2, 0.2)), 0.2, 1.0),
        "thermal_anomaly": centred(streams_of[6], (VERTICAL_TIERS, ZONAL_POINTS, MERIDIONAL_NODES), 1.0, 6.0, ((1, 16), (2, 8)), jnp.float32),
        "particle_class_map": touch_ends(jax.random.randint(streams_of[7], (ZONAL_POINTS, MERIDIONAL_NODES), 0, NBIN), jax.random.fold_in(streams_of[7], 1), 0, NBIN - 1).astype(jnp.int32),
        "ground_cover_kind": touch_ends(jax.random.randint(streams_of[8], (ZONAL_POINTS, MERIDIONAL_NODES), 0, NLU), jax.random.fold_in(streams_of[8], 1), 0, NLU - 1).astype(jnp.int32),
        "arid_extinction_table": jnp.clip(jax.random.uniform(streams_of[9], (S, 2 * NBIN * NW), jnp.float32, 0.0, 0.015625), 0.0, 0.015625).astype(jnp.bfloat16),
        "swelling_factors": jnp.clip(jax.random.uniform(streams_of[10], (S, 2 * NBIN * NW), jnp.float32, 0.0, 0.00390625), 0.0, 0.00390625).astype(jnp.bfloat16),
        "settling_velocities": jnp.clip(jnp.exp(jax.random.uniform(streams_of[11], (NLU, S), jnp.float32, math.log(0.05), math.log(2.0))), 0.05, 2.0),
        "arriving_irradiance": jnp.clip(jnp.exp(jax.random.uniform(streams_of[12], (NW,), jnp.float32, math.log(0.5), math.log(2.0))), 0.5, 2.0),
    }


SPREAD_FACTOR = 0.2
group_width = 16


def upwind(tracer, west_side, east_side, south_side, north_side, east_courant, north_courant):
    return (tracer - jnp.maximum(east_courant, 0.0) * (tracer - west_side)
            - jnp.minimum(east_courant, 0.0) * (east_side - tracer)
            - jnp.maximum(north_courant, 0.0) * (tracer - south_side)
            - jnp.minimum(north_courant, 0.0) * (north_side - tracer))


def radiate(optical, cosine, sunlight):
    layers_count = optical.shape[0]
    wavelengths = optical.shape[1] // 2
    weights = sunlight.reshape((wavelengths,) + (1,) * (optical.ndim - 2))
    overhead = jnp.zeros_like(optical[0, :wavelengths])
    layers = [None] * layers_count
    for height in reversed(range(layers_count)):
        transmitted = jnp.exp(-overhead / cosine)
        layers[height] = cosine * jnp.sum(weights * optical[height, wavelengths:] * transmitted, axis=0)
        overhead = overhead + optical[height, :wavelengths]
    return jnp.stack(layers)


def reference(tracer_amounts, zonal_transit_ratio, meridional_transit_ratio, moisture_ratio, stratum_depths, sun_elevation_factor, thermal_anomaly,
              particle_class_map, ground_cover_kind, arid_extinction_table, swelling_factors, settling_velocities, arriving_irradiance):
    group_count = S // group_width
    columns_all = 4 * NBIN * NW
    half_cols = 2 * NBIN * NW
    table_all = jnp.concatenate([arid_extinction_table, swelling_factors], axis=1).reshape(group_count, group_width, columns_all)
    velocity = jnp.moveaxis(settling_velocities.reshape(NLU, group_count, group_width), 1, 0)
    bin_mask = (particle_class_map[..., None] == jnp.arange(NBIN, dtype=jnp.int32)).astype(jnp.float32)
    level_outs = []
    optical_levels = []
    for height in range(VERTICAL_TIERS):
        east_courant = zonal_transit_ratio[height][..., None]
        north_courant = meridional_transit_ratio[height][..., None]
        groups = jnp.moveaxis(tracer_amounts[height].reshape(ZONAL_POINTS, MERIDIONAL_NODES, group_count, group_width), 2, 0)

        def advance_group(accumulated, members, height=height, east_courant=east_courant,
                          north_courant=north_courant):
            species_block, velocity_rows, table_rows = members
            tracer = species_block.astype(jnp.float32)
            for substep in range(SUB):
                padded = jnp.pad(tracer, ((1, 1), (0, 0), (0, 0)))
                padded_y = jnp.pad(tracer, ((0, 0), (1, 1), (0, 0)))
                tracer = upwind(tracer, padded[:-2], padded[2:], padded_y[:, :-2], padded_y[:, 2:],
                                east_courant, north_courant)
            if height == 0:
                loss_rate = velocity_rows[ground_cover_kind] / stratum_depths[0][..., None]
                tracer = tracer / (1.0 + loss_rate)
            rounded = tracer.astype(jnp.bfloat16)
            accumulated = accumulated + jnp.dot(rounded.reshape(ZONAL_POINTS * MERIDIONAL_NODES, group_width), table_rows,
                                                preferred_element_type=jnp.float32)
            return accumulated, tracer

        products, tracers = lax.scan(advance_group, jnp.zeros((ZONAL_POINTS * MERIDIONAL_NODES, columns_all), jnp.float32),
                                     (groups, velocity, table_all))
        level_outs.append(jnp.moveaxis(tracers, 0, 2).reshape(ZONAL_POINTS, MERIDIONAL_NODES, S))
        dry = products[:, :half_cols].reshape(ZONAL_POINTS, MERIDIONAL_NODES, NBIN, 2 * NW)
        wet = products[:, half_cols:].reshape(ZONAL_POINTS, MERIDIONAL_NODES, NBIN, 2 * NW)
        growth = moisture_ratio[height] / (1.0 - moisture_ratio[height])
        combined = dry + growth[..., None, None] * wet
        selected = jnp.sum(combined * bin_mask[..., None], axis=2)
        optical_levels.append(jnp.moveaxis(selected * stratum_depths[height][..., None], 2, 0))
    updated_tracer_amounts = jnp.stack(level_outs)
    optical = jnp.stack(optical_levels)
    warming_tendency = radiate(optical, sun_elevation_factor, arriving_irradiance)
    framed_thermal_field = jnp.pad(thermal_anomaly, ((0, 0), (1, 1), (1, 1)))
    second_difference_map = (framed_thermal_field[:, 2:, 1:-1] + framed_thermal_field[:, :-2, 1:-1] + framed_thermal_field[:, 1:-1, 2:]
               + framed_thermal_field[:, 1:-1, :-2] - 4.0 * thermal_anomaly)
    updated_thermal_anomaly = thermal_anomaly + SPREAD_FACTOR * second_difference_map + warming_tendency
    return updated_tracer_amounts, updated_thermal_anomaly
```

```python
import functools

import jax
import jax.numpy as jnp
import numpy as np
from jax import lax
from jax.experimental import pallas as pl
from jax.experimental.pallas import tpu as pltpu
from jax.sharding import PartitionSpec as P

SUB = 3
NBIN = 8
NW = 4
SPREAD_FACTOR = 0.2

LANES = 128
MARGIN = 16
RIM = 2
CHUNKS = (256, 256, 256, 256)

UV_ROWS = 24
MOIST_ROW = 48
DEPTH_ROW = 64
SUN_ROW = 80
EDGE_ROW = 88
FIELD_ROWS = 96


def spread_matrix():
    field = np.full((LANES,), -1)
    for k in range(72):
        field[k] = k % 24
    for k in range(24):
        field[72 + k] = 24 + k % 8
    field[96:104] = 32 + np.arange(8)
    out = np.zeros((20, LANES, 2 * LANES), np.float32)
    for k in range(LANES):
        if field[k] >= 0:
            half = field[k] % 2
            out[field[k] // 2, k, half * LANES : (half + 1) * LANES] = 1.0
    return out


def three_parts(x):
    high = x.astype(jnp.bfloat16).astype(jnp.float32)
    rest = x - high
    middle = rest.astype(jnp.bfloat16).astype(jnp.float32)
    return [high, middle, rest - middle]


def pack_kernel(place, u, v, moisture, depth, sun, warmth, low, high, out, ext):
    mine = place[0]
    parts = u.shape[1] // 8
    for f in range(4):
        source = (u, v)[f // 2]
        ext[f, 8 : 8 + u.shape[1], :] = source[f % 2]
        ext[f, 8 - RIM : 8, :] = low[RIM * f : RIM * (f + 1), :]
        ext[f, 8 + u.shape[1] : 8 + u.shape[1] + RIM, :] = high[RIM * f : RIM * (f + 1), :]
    turned = warmth[...].reshape(2 * u.shape[1], LANES).T
    last = turned[LANES - 1 :, :]
    initial = turned[:1, :]
    wide = 8 + 2 * RIM
    for d in range(parts):
        for level in range(2):
            base = UV_ROWS * level
            out[d, base : base + wide, :] = ext[level, 8 * d + 8 - RIM : 8 * d + 16 + RIM, :]
            out[d, base + wide : base + 2 * wide, :] = ext[
                2 + level, 8 * d + 8 - RIM : 8 * d + 16 + RIM, :
            ]
            out[d, MOIST_ROW + 8 * level : MOIST_ROW + 8 * level + 8, :] = moisture[
                level, 8 * d : 8 * d + 8, :
            ]
            out[d, DEPTH_ROW + 8 * level : DEPTH_ROW + 8 * level + 8, :] = depth[
                level, 8 * d : 8 * d + 8, :
            ]
        out[d, SUN_ROW : SUN_ROW + 8, :] = sun[8 * d : 8 * d + 8, :]
        row = jnp.where(mine + 1 == d, last, jnp.where(mine - 1 == d, initial, 0.0))
        out[d, EDGE_ROW : EDGE_ROW + 8, :] = jnp.broadcast_to(row, (8, LANES))


def warm_kernel(place, warmth, low, high, left, right, out, ext):
    span = warmth.shape[1]
    lane = lax.broadcasted_iota(jnp.int32, (span, LANES), 1)
    for level in range(2):
        here = warmth[level]
        ext[8 : 8 + span, :] = here
        ext[7:8, :] = low[level : level + 1, :]
        ext[8 + span : 9 + span, :] = high[level : level + 1, :]
        left_rows = jnp.broadcast_to(left[:, level * span : (level + 1) * span], (LANES, span)).T
        right_rows = jnp.broadcast_to(right[:, level * span : (level + 1) * span], (LANES, span)).T
        west = jnp.where(lane == 0, left_rows, pltpu.roll(here, 1, 1))
        east = jnp.where(lane == LANES - 1, right_rows, pltpu.roll(here, LANES - 1, 1))
        laplace = ext[9 : 9 + span, :] + ext[7 : 7 + span, :] + east + west - 4.0 * here
        out[level] = here + SPREAD_FACTOR * laplace


def row_blocks(first, count, size=64):
    blocks = []
    while count > 0:
        take = size if count >= 2 * size or count == size else min(count, 2 * size - 8)
        if take > size + 32:
            take = (take // 2 + 7) // 8 * 8
        blocks.append((first, take))
        first += take
        count -= take
    return blocks


def chunk_kernel(start, rows, grid_rows, first, final, *refs):
    refs = list(refs)
    zero, sunlight, fields, kind, bins, spread, table, speeds, tracer = refs[:9]
    del refs[:9]
    west, east = refs[:2]
    del refs[:2]
    if not first:
        west_before, east_before = refs[:2]
        del refs[:4]
    out, heat = refs[:2]
    wide_in, even, odd, coef, turned, result, thick, warm, classes = refs[2:11]
    in_sems, out_sems, heat_sem = refs[11:]

    stop = start + rows
    span = rows + 2 * MARGIN
    blocks = rows // LANES
    first_block = start // LANES
    low = 0 if first else start - MARGIN
    top = grid_rows if final else stop + MARGIN
    offset = low - (start - MARGIN)
    filled = top - low
    columns = 8
    wide = columns + 2 * SUB
    z = zero[0]

    copies = []
    for level in (0, 1):
        rims_at = 2 * MARGIN if not first else MARGIN
        length = west.shape[2]
        these = [
            pltpu.make_async_copy(
                tracer.at[level, :, low:top, :],
                wide_in.at[level, SUB : SUB + columns, offset : offset + filled, :],
                in_sems.at[level, 0],
            ),
            pltpu.make_async_copy(
                west.at[level],
                wide_in.at[level, 0:SUB, rims_at : rims_at + length, :],
                in_sems.at[level, 1],
            ),
            pltpu.make_async_copy(
                east.at[level],
                wide_in.at[level, SUB + columns : wide, rims_at : rims_at + length, :],
                in_sems.at[level, 2],
            ),
        ]
        if not first:
            before = west_before.shape[2]
            these.append(
                pltpu.make_async_copy(
                    west_before.at[level, :, before - 2 * MARGIN : before, :],
                    wide_in.at[level, 0:SUB, 0 : 2 * MARGIN, :],
                    in_sems.at[level, 3],
                )
            )
            these.append(
                pltpu.make_async_copy(
                    east_before.at[level, :, before - 2 * MARGIN : before, :],
                    wide_in.at[level, SUB + columns : wide, 0 : 2 * MARGIN, :],
                    in_sems.at[level, 4],
                )
            )
        copies.append(these)
    for level in (1, 0):
        for copy in copies[level]:
            copy.start()

    for b in range(blocks):
        classes[b] = bins[:, start + b * LANES : start + (b + 1) * LANES]
    sublane = lax.broadcasted_iota(jnp.int32, (8, LANES), 0)
    weights = jnp.zeros((8, LANES), jnp.float32)
    for w in range(NW):
        weights = jnp.where(sublane == NW + w, sunlight[w], weights)
    lane = lax.broadcasted_iota(jnp.int32, (1, LANES), 1)
    category = jnp.where(lane < 72, lane % 24, -1).astype(jnp.float32)

    def turn(block, level):
        parts = three_parts(fields[block, UV_ROWS * level : UV_ROWS * (level + 1), :])
        if level == 0:
            parts += three_parts(fields[block, DEPTH_ROW : DEPTH_ROW + 8, :])
            parts.append(kind[:, block * LANES : (block + 1) * LANES].astype(jnp.float32))
            parts.append(jnp.zeros((24, LANES), jnp.float32))
        else:
            parts.append(jnp.zeros((56, LANES), jnp.float32))
        return jnp.concatenate(parts, axis=0).T.astype(jnp.bfloat16)

    def step(source, c, i, r0, count):
        here = source[c, r0 : r0 + count, :]
        u = coef[i, r0 : r0 + count, :]
        v = coef[12 + i, r0 : r0 + count, :]
        across = jnp.where(
            u > 0.0, source[c - 1, r0 : r0 + count, :], source[c + 1, r0 : r0 + count, :]
        )
        along = jnp.where(
            v > 0.0,
            source[c, pl.ds(z + (r0 - 1), count), :],
            source[c, pl.ds(z + (r0 + 1), count), :],
        )
        return here - jnp.abs(u) * (here - across) - jnp.abs(v) * (here - along)

    out_copies = []
    for level in (1, 0):
        for j in range(-1, blocks + 1):
            block = first_block + j
            if j == -1:
                if first:
                    turned[0:MARGIN, :] = jnp.zeros((MARGIN, LANES), jnp.bfloat16)
                else:
                    turned[0:MARGIN, :] = turn(block, level)[LANES - MARGIN :, :]
            elif j == blocks:
                at = MARGIN + rows
                if final:
                    turned[at : at + MARGIN, :] = jnp.zeros((MARGIN, LANES), jnp.bfloat16)
                else:
                    turned[at : at + MARGIN, :] = turn(block, level)[:MARGIN, :]
            else:
                at = MARGIN + LANES * j
                turned[at : at + LANES, :] = turn(block, level)

        def spread_pair(p, carry):
            both = jnp.dot(turned[...], spread[p], preferred_element_type=jnp.float32)
            coef[2 * p] = both[:, :LANES]
            coef[2 * p + 1] = both[:, LANES:]
            return carry

        lax.fori_loop(0, 20 if level == 0 else 12, spread_pair, 0)

        for copy in copies[level]:
            copy.wait()

        def widen(c, carry):
            even[c, offset : offset + filled, :] = wide_in[
                level, c, offset : offset + filled, :
            ].astype(jnp.float32)
            if first:
                even[c, 0:MARGIN, :] = jnp.zeros((MARGIN, LANES), jnp.float32)
            if final:
                even[c, span - MARGIN :, :] = jnp.zeros((MARGIN, LANES), jnp.float32)
            return carry

        lax.fori_loop(0, wide, widen, 0)

        def substep_one(c, carry):
            for r0, count in row_blocks(8, span - 16):
                odd[c, r0 : r0 + count, :] = step(even, c, c - 1, r0, count)
            return carry

        def substep_two(c, carry):
            for r0, count in row_blocks(8, span - 16):
                even[c, r0 : r0 + count, :] = step(odd, c, c - 1, r0, count)
            return carry

        lax.fori_loop(1, wide - 1, substep_one, 0)
        lax.fori_loop(2, wide - 2, substep_two, 0)

        def finish(x, carry):
            c = x + SUB
            for r0, count in row_blocks(MARGIN, rows):
                tracer_now = step(even, c, c - 1, r0, count)
                if level == 0:
                    depth = coef[24 + x, r0 : r0 + count, :]
                    hot = jnp.where(coef[32 + x, r0 : r0 + count, :] == category, 1.0, 0.0)
                    speed = jnp.dot(
                        hot.astype(jnp.bfloat16), speeds[...], preferred_element_type=jnp.float32
                    )
                    tracer_now = tracer_now * depth / (depth + speed)
                result[level, x, r0 - MARGIN : r0 - MARGIN + count, :] = tracer_now
            rounded = result[level, x, :, :].astype(jnp.bfloat16)
            projected = lax.dot_general(
                table[...], rounded, (((1,), (1,)), ((), ())), preferred_element_type=jnp.float32
            )
            for b in range(blocks):
                block = first_block + b
                which = classes[b, pl.ds(x, 1), :]
                dry = jnp.zeros((8, LANES), jnp.float32)
                wet = jnp.zeros((8, LANES), jnp.float32)
                for k in range(NBIN):
                    chosen = which == k
                    lanes = slice(b * LANES, (b + 1) * LANES)
                    dry = jnp.where(chosen, projected[8 * k : 8 * k + 8, lanes], dry)
                    wet = jnp.where(chosen, projected[64 + 8 * k : 72 + 8 * k, lanes], wet)
                moist = fields[block, pl.ds(MOIST_ROW + 8 * level + x, 1), :]
                depth_row = fields[block, pl.ds(DEPTH_ROW + 8 * level + x, 1), :]
                sun = fields[block, pl.ds(SUN_ROW + x, 1), :]
                growth = moist / (1.0 - moist)
                optical = (dry + growth * wet) * depth_row
                if level == 1:
                    thick[x, b] = optical
                    lit = weights * optical
                else:
                    overhead = pltpu.roll(thick[x, b], NW, 0)
                    lit = weights * optical * jnp.exp(-overhead / sun)
                warm[b, pl.ds(8 * level + x, 1), :] = sun * jnp.sum(lit, axis=0, keepdims=True)
            return carry

        lax.fori_loop(0, columns, finish, 0)
        copy = pltpu.make_async_copy(
            result.at[level], out.at[level, :, start:stop, :], out_sems.at[level]
        )
        copy.start()
        out_copies.append(copy)

    copy = pltpu.make_async_copy(warm, heat.at[first_block : first_block + blocks], heat_sem.at[0])
    copy.start()
    out_copies.append(copy)
    for copy in out_copies:
        copy.wait()


def per_device(
    tracer_amounts,
    zonal_transit_ratio,
    meridional_transit_ratio,
    moisture_ratio,
    stratum_depths,
    sun_elevation_factor,
    thermal_anomaly,
    particle_class_map,
    ground_cover_kind,
    arid_extinction_table,
    swelling_factors,
    settling_velocities,
    arriving_irradiance,
):
    f32, bf16 = jnp.float32, jnp.bfloat16
    levels, columns, grid_rows, species = tracer_amounts.shape
    tile = thermal_anomaly.shape[1]
    gx, gy = lax.axis_size("gx"), lax.axis_size("gy")
    strips = ("gx", "gy")
    up = [(i, i + 1) for i in range(gx * gy - 1)]
    down = [(j, i) for i, j in up]
    gx_up = [(i, i + 1) for i in range(gx - 1)]
    gx_down = [(j, i) for i, j in gx_up]
    vmem = pl.BlockSpec(memory_space=pltpu.VMEM)
    smem = pl.BlockSpec(memory_space=pltpu.SMEM)
    hbm = pl.BlockSpec(memory_space=pltpu.HBM)

    bounds = [0]
    for rows in CHUNKS:
        bounds.append(bounds[-1] + rows)
    cuts = [0] + [b + MARGIN for b in bounds[1:-1]] + [grid_rows]
    wests, easts = [], []
    for low, top in zip(cuts[:-1], cuts[1:]):
        wests.append(lax.ppermute(tracer_amounts[:, columns - SUB :, low:top], strips, up))
        easts.append(lax.ppermute(tracer_amounts[:, :SUB, low:top], strips, down))

    def edge(pick, row):
        cut = [a[:, pick].reshape(-1, LANES) for a in (zonal_transit_ratio, meridional_transit_ratio)]
        return jnp.concatenate(cut + [thermal_anomaly[:, row]], axis=0)

    from_low = lax.ppermute(edge(slice(tile - RIM, tile), tile - 1), "gx", gx_up)
    from_high = lax.ppermute(edge(slice(0, RIM), 0), "gx", gx_down)

    mine = lax.axis_index("gy")
    place = mine.astype(jnp.int32).reshape(1)
    packed = pl.pallas_call(
        pack_kernel,
        out_shape=jax.ShapeDtypeStruct((gy, FIELD_ROWS, LANES), f32),
        in_specs=[smem] + [vmem] * 8,
        out_specs=vmem,
        scratch_shapes=[pltpu.VMEM((4, tile + 16, LANES), f32)],
        name="pack",
    )(
        place,
        zonal_transit_ratio,
        meridional_transit_ratio,
        moisture_ratio,
        stratum_depths,
        sun_elevation_factor,
        thermal_anomaly,
        from_low[: 4 * RIM],
        from_high[: 4 * RIM],
    )
    fields = lax.all_to_all(packed, "gy", split_axis=0, concat_axis=0, tiled=True)

    def rim_row(source):
        return lax.dynamic_slice(fields, (source, EDGE_ROW, 0), (1, 1, LANES)).reshape(1, LANES)

    warmed = pl.pallas_call(
        warm_kernel,
        out_shape=jax.ShapeDtypeStruct(thermal_anomaly.shape, f32),
        in_specs=[smem] + [vmem] * 5,
        out_specs=vmem,
        scratch_shapes=[pltpu.VMEM((tile + 16, LANES), f32)],
        name="warm",
    )(
        place,
        thermal_anomaly,
        from_low[4 * RIM :],
        from_high[4 * RIM :],
        rim_row(jnp.maximum(mine - 1, 0)),
        rim_row(jnp.minimum(mine + 1, gy - 1)),
    )

    spread = jnp.asarray(spread_matrix(), bf16)
    table = jnp.concatenate([arid_extinction_table, swelling_factors], axis=1).T
    parts, rest = [], settling_velocities
    for _ in range(3):
        part = lax.reduce_precision(rest, 8, 7)
        parts.append(part.astype(bf16))
        rest = rest - part
    parts.append(jnp.zeros((LANES - 3 * settling_velocities.shape[0], species), bf16))
    speeds = jnp.concatenate(parts, axis=0)
    zero = jnp.zeros((1,), jnp.int32)

    out = heat = None
    for k, rows in enumerate(CHUNKS):
        first, final = k == 0, k == len(CHUNKS) - 1
        span = rows + 2 * MARGIN
        operands = [
            zero,
            arriving_irradiance,
            fields,
            ground_cover_kind,
            particle_class_map,
            spread,
            table,
            speeds,
            tracer_amounts,
            wests[k],
            easts[k],
        ]
        specs = [smem, smem] + [vmem] * 6 + [hbm] * 3
        aliases = {}
        if not first:
            operands += [wests[k - 1], easts[k - 1], out, heat]
            specs += [hbm] * 4
            aliases = {13: 0, 14: 1}
        work = rows * columns * levels * species
        out, heat = pl.pallas_call(
            functools.partial(chunk_kernel, bounds[k], rows, grid_rows, first, final),
            out_shape=(
                jax.ShapeDtypeStruct(tracer_amounts.shape, f32),
                jax.ShapeDtypeStruct((gy, levels * columns, LANES), f32),
            ),
            in_specs=specs,
            out_specs=(hbm, hbm),
            scratch_shapes=[
                pltpu.VMEM((levels, columns + 2 * SUB, span, LANES), bf16),
                pltpu.VMEM((columns + 2 * SUB, span, LANES), f32),
                pltpu.VMEM((columns + 2 * SUB, span, LANES), f32),
                pltpu.VMEM((40, span, LANES), f32),
                pltpu.VMEM((span, LANES), bf16),
                pltpu.VMEM((levels, columns, rows, LANES), f32),
                pltpu.VMEM((columns, rows // LANES, 8, LANES), f32),
                pltpu.VMEM((rows // LANES, levels * columns, LANES), f32),
                pltpu.VMEM((rows // LANES, columns, LANES), jnp.int32),
                pltpu.SemaphoreType.DMA((levels, 5)),
                pltpu.SemaphoreType.DMA((levels,)),
                pltpu.SemaphoreType.DMA((1,)),
            ],
            input_output_aliases=aliases,
            compiler_params=pltpu.CompilerParams(vmem_limit_bytes=40 * 1024 * 1024),
            cost_estimate=pl.CostEstimate(
                flops=60 * work, transcendentals=0, bytes_accessed=8 * work
            ),
            name="chunk%d" % k,
        )(*operands)

    returned = lax.all_to_all(heat, "gy", split_axis=0, concat_axis=0, tiled=True)
    returned = returned.reshape(gy, levels, columns, LANES).transpose(1, 0, 2, 3)
    return out, warmed + returned.reshape(thermal_anomaly.shape)


def solution(mesh):
    return jax.shard_map(
        per_device,
        mesh=mesh,
        in_specs=(
            P(None, ("gx", "gy"), None, None),
            P(None, "gx", "gy"),
            P(None, "gx", "gy"),
            P(None, "gx", "gy"),
            P(None, "gx", "gy"),
            P("gx", "gy"),
            P(None, "gx", "gy"),
            P(("gx", "gy"), None),
            P(("gx", "gy"), None),
            P(),
            P(),
            P(),
            P(),
        ),
        out_specs=(P(None, ("gx", "gy"), None, None), P(None, "gx", "gy")),
        check_vma=False,
    )
```

```python
import functools

import jax
import jax.numpy as jnp
import numpy as np
from jax import lax
from jax.experimental import pallas as pl
from jax.experimental.pallas import tpu as pltpu
from jax.sharding import PartitionSpec as P


SUB = 3
NBIN = 8
NW = 4
SPREAD_FACTOR = 0.2

LANES = 128
MARGIN = 16
RIM = 2
CHUNKS = (384, 256, 256, 128)

UV_ROWS = 24
MOIST_ROW = 48
DEPTH_ROW = 64
SUN_ROW = 80
EDGE_ROW = 88
FIELD_ROWS = 96


def spread_matrix():
    field = np.full((LANES,), -1)
    for k in range(72):
        field[k] = k % 24
    for k in range(24):
        field[72 + k] = 24 + k % 8
    field[96:104] = 32 + np.arange(8)
    out = np.zeros((20, LANES, 2 * LANES), np.float32)
    for k in range(LANES):
        if field[k] >= 0:
            half = field[k] % 2
            out[field[k] // 2, k, half * LANES : (half + 1) * LANES] = 1.0
    return out


def three_parts(x):
    high = x.astype(jnp.bfloat16).astype(jnp.float32)
    rest = x - high
    middle = rest.astype(jnp.bfloat16).astype(jnp.float32)
    return [high, middle, rest - middle]


def pack_kernel(place, u, v, moisture, depth, sun, warmth, low, high, out, ext):
    mine = place[0]
    parts = u.shape[1] // 8
    for f in range(4):
        source = (u, v)[f // 2]
        ext[f, 8 : 8 + u.shape[1], :] = source[f % 2]
        ext[f, 8 - RIM : 8, :] = low[RIM * f : RIM * (f + 1), :]
        ext[f, 8 + u.shape[1] : 8 + u.shape[1] + RIM, :] = high[RIM * f : RIM * (f + 1), :]
    turned = warmth[...].reshape(2 * u.shape[1], LANES).T
    last = turned[LANES - 1 :, :]
    initial = turned[:1, :]
    wide = 8 + 2 * RIM
    for d in range(parts):
        for level in range(2):
            base = UV_ROWS * level
            out[d, base : base + wide, :] = ext[level, 8 * d + 8 - RIM : 8 * d + 16 + RIM, :]
            out[d, base + wide : base + 2 * wide, :] = ext[
                2 + level, 8 * d + 8 - RIM : 8 * d + 16 + RIM, :
            ]
            out[d, MOIST_ROW + 8 * level : MOIST_ROW + 8 * level + 8, :] = moisture[
                level, 8 * d : 8 * d + 8, :
            ]
            out[d, DEPTH_ROW + 8 * level : DEPTH_ROW + 8 * level + 8, :] = depth[
                level, 8 * d : 8 * d + 8, :
            ]
        out[d, SUN_ROW : SUN_ROW + 8, :] = sun[8 * d : 8 * d + 8, :]
        row = jnp.where(mine + 1 == d, last, jnp.where(mine - 1 == d, initial, 0.0))
        out[d, EDGE_ROW : EDGE_ROW + 8, :] = jnp.broadcast_to(row, (8, LANES))


def warm_kernel(place, warmth, low, high, left, right, out, ext):
    span = warmth.shape[1]
    lane = lax.broadcasted_iota(jnp.int32, (span, LANES), 1)
    for level in range(2):
        here = warmth[level]
        ext[8 : 8 + span, :] = here
        ext[7:8, :] = low[level : level + 1, :]
        ext[8 + span : 9 + span, :] = high[level : level + 1, :]
        left_rows = jnp.broadcast_to(left[:, level * span : (level + 1) * span], (LANES, span)).T
        right_rows = jnp.broadcast_to(right[:, level * span : (level + 1) * span], (LANES, span)).T
        west = jnp.where(lane == 0, left_rows, pltpu.roll(here, 1, 1))
        east = jnp.where(lane == LANES - 1, right_rows, pltpu.roll(here, LANES - 1, 1))
        laplace = ext[9 : 9 + span, :] + ext[7 : 7 + span, :] + east + west - 4.0 * here
        out[level] = here + SPREAD_FACTOR * laplace


def row_blocks(first, count, size=64):
    blocks = []
    while count > 0:
        take = size if count >= 2 * size or count == size else min(count, 2 * size - 8)
        if take > size + 32:
            take = (take // 2 + 7) // 8 * 8
        blocks.append((first, take))
        first += take
        count -= take
    return blocks


def chunk_kernel(start, rows, grid_rows, first, final, *refs):
    refs = list(refs)
    zero, sunlight, fields, kind, bins, spread, table, speeds, tracer = refs[:9]
    del refs[:9]
    west, east = refs[:2]
    del refs[:2]
    if not first:
        west_before, east_before = refs[:2]
        del refs[:4]
    out, heat = refs[:2]
    even, odd, coef, turned, result, thick, warm, out_sems, heat_sem = refs[2:]

    stop = start + rows
    span = rows + 2 * MARGIN
    blocks = rows // LANES
    first_block = start // LANES
    low = 0 if first else start - MARGIN
    top = grid_rows if final else stop + MARGIN
    offset = low - (start - MARGIN)
    filled = top - low
    columns = 8
    wide = columns + 2 * SUB
    z = zero[0]

    sublane = lax.broadcasted_iota(jnp.int32, (8, LANES), 0)
    weights = jnp.zeros((8, LANES), jnp.float32)
    for w in range(NW):
        weights = jnp.where(sublane == NW + w, sunlight[w], weights)
    lane = lax.broadcasted_iota(jnp.int32, (1, LANES), 1)
    category = jnp.where(lane < 72, lane % 24, -1).astype(jnp.float32)

    def turn(block, level):
        parts = three_parts(fields[block, UV_ROWS * level : UV_ROWS * (level + 1), :])
        if level == 0:
            parts += three_parts(fields[block, DEPTH_ROW : DEPTH_ROW + 8, :])
            parts.append(kind[:, block * LANES : (block + 1) * LANES].astype(jnp.float32))
            parts.append(jnp.zeros((24, LANES), jnp.float32))
        else:
            parts.append(jnp.zeros((56, LANES), jnp.float32))
        return jnp.concatenate(parts, axis=0).T.astype(jnp.bfloat16)

    def row(block, at):
        return fields[block, at : at + 1, :]

    def step(source, c, i, r0, count):
        here = source[c, r0 : r0 + count, :]
        u = coef[i, r0 : r0 + count, :]
        v = coef[12 + i, r0 : r0 + count, :]
        across = jnp.where(
            u > 0.0, source[c - 1, r0 : r0 + count, :], source[c + 1, r0 : r0 + count, :]
        )
        along = jnp.where(
            v > 0.0,
            source[c, pl.ds(z + (r0 - 1), count), :],
            source[c, pl.ds(z + (r0 + 1), count), :],
        )
        return here - jnp.abs(u) * (here - across) - jnp.abs(v) * (here - along)

    out_copies = []
    for level in (1, 0):
        for j in range(-1, blocks + 1):
            block = first_block + j
            if j == -1:
                if first:
                    turned[0:MARGIN, :] = jnp.zeros((MARGIN, LANES), jnp.bfloat16)
                else:
                    turned[0:MARGIN, :] = turn(block, level)[LANES - MARGIN :, :]
            elif j == blocks:
                at = MARGIN + rows
                if final:
                    turned[at : at + MARGIN, :] = jnp.zeros((MARGIN, LANES), jnp.bfloat16)
                else:
                    turned[at : at + MARGIN, :] = turn(block, level)[:MARGIN, :]
            else:
                at = MARGIN + LANES * j
                turned[at : at + LANES, :] = turn(block, level)

        lhs = turned[...]
        for p in range(20 if level == 0 else 12):
            both = jnp.dot(lhs, spread[p], preferred_element_type=jnp.float32)
            coef[2 * p] = both[:, :LANES]
            coef[2 * p + 1] = both[:, LANES:]

        rims_at = MARGIN if first else 2 * MARGIN
        length = west.shape[2]

        def widen_rims(c, carry):
            for at, rim, before in (
                (c, west, None if first else west_before),
                (SUB + columns + c, east, None if first else east_before),
            ):
                if first:
                    even[at, 0:MARGIN, :] = jnp.zeros((MARGIN, LANES), jnp.float32)
                else:
                    end = before.shape[2]
                    even[at, 0 : 2 * MARGIN, :] = before[
                        level, c, end - 2 * MARGIN : end, :
                    ].astype(jnp.float32)
                even[at, rims_at : rims_at + length, :] = rim[level, c].astype(jnp.float32)
                if final:
                    even[at, span - MARGIN :, :] = jnp.zeros((MARGIN, LANES), jnp.float32)
            return carry

        def widen(c, carry):
            even[SUB + c, offset : offset + filled, :] = tracer[level, c, low:top, :].astype(
                jnp.float32
            )
            if first:
                even[SUB + c, 0:MARGIN, :] = jnp.zeros((MARGIN, LANES), jnp.float32)
            if final:
                even[SUB + c, span - MARGIN :, :] = jnp.zeros((MARGIN, LANES), jnp.float32)
            return carry

        lax.fori_loop(0, SUB, widen_rims, 0)
        lax.fori_loop(0, columns, widen, 0)

        def substep_one(c, carry):
            for r0, count in row_blocks(8, span - 16):
                odd[c, r0 : r0 + count, :] = step(even, c, c - 1, r0, count)
            return carry

        def substep_two(c, carry):
            for r0, count in row_blocks(8, span - 16):
                even[c, r0 : r0 + count, :] = step(odd, c, c - 1, r0, count)
            return carry

        lax.fori_loop(1, wide - 1, substep_one, 0)
        lax.fori_loop(2, wide - 2, substep_two, 0)

        for x in range(columns):
            c = x + SUB
            for r0, count in row_blocks(MARGIN, rows):
                tracer_now = step(even, c, c - 1, r0, count)
                if level == 0:
                    depth = coef[24 + x, r0 : r0 + count, :]
                    hot = jnp.where(coef[32 + x, r0 : r0 + count, :] == category, 1.0, 0.0)
                    speed = jnp.dot(
                        hot.astype(jnp.bfloat16), speeds[...], preferred_element_type=jnp.float32
                    )
                    tracer_now = tracer_now * depth / (depth + speed)
                result[level, x, r0 - MARGIN : r0 - MARGIN + count, :] = tracer_now
            rounded = result[level, x, :, :].astype(jnp.bfloat16)
            projected = lax.dot_general(
                table[...], rounded, (((1,), (1,)), ((), ())), preferred_element_type=jnp.float32
            )
            for b in range(blocks):
                block = first_block + b
                which = bins[x : x + 1, block * LANES : (block + 1) * LANES]
                dry = jnp.zeros((8, LANES), jnp.float32)
                wet = jnp.zeros((8, LANES), jnp.float32)
                for k in range(NBIN):
                    chosen = which == k
                    lanes = slice(b * LANES, (b + 1) * LANES)
                    dry = jnp.where(chosen, projected[8 * k : 8 * k + 8, lanes], dry)
                    wet = jnp.where(chosen, projected[64 + 8 * k : 72 + 8 * k, lanes], wet)
                moist = row(block, MOIST_ROW + 8 * level + x)
                depth_row = row(block, DEPTH_ROW + 8 * level + x)
                sun = row(block, SUN_ROW + x)
                growth = moist / (1.0 - moist)
                optical = (dry + growth * wet) * depth_row
                if level == 1:
                    thick[x, b] = optical
                    lit = weights * optical
                else:
                    overhead = pltpu.roll(thick[x, b], NW, 0)
                    lit = weights * optical * jnp.exp(-overhead / sun)
                at = 8 * level + x
                warm[b, at : at + 1, :] = sun * jnp.sum(lit, axis=0, keepdims=True)
        copy = pltpu.make_async_copy(
            result.at[level], out.at[level, :, start:stop, :], out_sems.at[level]
        )
        copy.start()
        out_copies.append(copy)

    copy = pltpu.make_async_copy(warm, heat.at[first_block : first_block + blocks], heat_sem.at[0])
    copy.start()
    out_copies.append(copy)
    for copy in out_copies:
        copy.wait()


def per_device(
    tracer_amounts,
    zonal_transit_ratio,
    meridional_transit_ratio,
    moisture_ratio,
    stratum_depths,
    sun_elevation_factor,
    thermal_anomaly,
    particle_class_map,
    ground_cover_kind,
    arid_extinction_table,
    swelling_factors,
    settling_velocities,
    arriving_irradiance,
):
    f32, bf16 = jnp.float32, jnp.bfloat16
    levels, columns, grid_rows, species = tracer_amounts.shape
    tile = thermal_anomaly.shape[1]
    gx, gy = lax.axis_size("gx"), lax.axis_size("gy")
    strips = ("gx", "gy")
    up = [(i, i + 1) for i in range(gx * gy - 1)]
    down = [(j, i) for i, j in up]
    gx_up = [(i, i + 1) for i in range(gx - 1)]
    gx_down = [(j, i) for i, j in gx_up]
    vmem = pl.BlockSpec(memory_space=pltpu.VMEM)
    smem = pl.BlockSpec(memory_space=pltpu.SMEM)
    hbm = pl.BlockSpec(memory_space=pltpu.HBM)

    bounds = [0]
    for rows in CHUNKS:
        bounds.append(bounds[-1] + rows)
    cuts = [0] + [b + MARGIN for b in bounds[1:-1]] + [grid_rows]
    wests, easts = [], []
    for low, top in zip(cuts[:-1], cuts[1:]):
        wests.append(lax.ppermute(tracer_amounts[:, columns - SUB :, low:top], strips, up))
        easts.append(lax.ppermute(tracer_amounts[:, :SUB, low:top], strips, down))

    def edge(pick, row):
        cut = [a[:, pick].reshape(-1, LANES) for a in (zonal_transit_ratio, meridional_transit_ratio)]
        return jnp.concatenate(cut + [thermal_anomaly[:, row]], axis=0)

    from_low = lax.ppermute(edge(slice(tile - RIM, tile), tile - 1), "gx", gx_up)
    from_high = lax.ppermute(edge(slice(0, RIM), 0), "gx", gx_down)

    mine = lax.axis_index("gy")
    place = mine.astype(jnp.int32).reshape(1)
    packed = pl.pallas_call(
        pack_kernel,
        out_shape=jax.ShapeDtypeStruct((gy, FIELD_ROWS, LANES), f32),
        in_specs=[smem] + [vmem] * 8,
        out_specs=vmem,
        scratch_shapes=[pltpu.VMEM((4, tile + 16, LANES), f32)],
        name="pack",
    )(
        place,
        zonal_transit_ratio,
        meridional_transit_ratio,
        moisture_ratio,
        stratum_depths,
        sun_elevation_factor,
        thermal_anomaly,
        from_low[: 4 * RIM],
        from_high[: 4 * RIM],
    )
    fields = lax.all_to_all(packed, "gy", split_axis=0, concat_axis=0, tiled=True)

    def rim_row(source):
        return lax.dynamic_slice(fields, (source, EDGE_ROW, 0), (1, 1, LANES)).reshape(1, LANES)

    warmed = pl.pallas_call(
        warm_kernel,
        out_shape=jax.ShapeDtypeStruct(thermal_anomaly.shape, f32),
        in_specs=[smem] + [vmem] * 5,
        out_specs=vmem,
        scratch_shapes=[pltpu.VMEM((tile + 16, LANES), f32)],
        name="warm",
    )(
        place,
        thermal_anomaly,
        from_low[4 * RIM :],
        from_high[4 * RIM :],
        rim_row(jnp.maximum(mine - 1, 0)),
        rim_row(jnp.minimum(mine + 1, gy - 1)),
    )

    spread = jnp.asarray(spread_matrix(), bf16)
    table = jnp.concatenate([arid_extinction_table, swelling_factors], axis=1).T
    parts, rest = [], settling_velocities
    for _ in range(3):
        part = lax.reduce_precision(rest, 8, 7)
        parts.append(part.astype(bf16))
        rest = rest - part
    parts.append(jnp.zeros((LANES - 3 * settling_velocities.shape[0], species), bf16))
    speeds = jnp.concatenate(parts, axis=0)
    zero = jnp.zeros((1,), jnp.int32)

    out = heat = None
    for k, rows in enumerate(CHUNKS):
        first, final = k == 0, k == len(CHUNKS) - 1
        span = rows + 2 * MARGIN
        operands = [
            zero,
            arriving_irradiance,
            fields,
            ground_cover_kind,
            particle_class_map,
            spread,
            table,
            speeds,
            tracer_amounts,
            wests[k],
            easts[k],
        ]
        specs = [smem, smem] + [vmem] * 9
        aliases = {}
        if not first:
            operands += [wests[k - 1], easts[k - 1], out, heat]
            specs += [vmem] * 2 + [hbm] * 2
            aliases = {13: 0, 14: 1}
        work = rows * columns * levels * species
        out, heat = pl.pallas_call(
            functools.partial(chunk_kernel, bounds[k], rows, grid_rows, first, final),
            out_shape=(
                jax.ShapeDtypeStruct(tracer_amounts.shape, f32),
                jax.ShapeDtypeStruct((gy, levels * columns, LANES), f32),
            ),
            in_specs=specs,
            out_specs=(hbm, hbm),
            scratch_shapes=[
                pltpu.VMEM((columns + 2 * SUB, span, LANES), f32),
                pltpu.VMEM((columns + 2 * SUB, span, LANES), f32),
                pltpu.VMEM((40, span, LANES), f32),
                pltpu.VMEM((span, LANES), bf16),
                pltpu.VMEM((levels, columns, rows, LANES), f32),
                pltpu.VMEM((columns, rows // LANES, 8, LANES), f32),
                pltpu.VMEM((rows // LANES, levels * columns, LANES), f32),
                pltpu.SemaphoreType.DMA((levels,)),
                pltpu.SemaphoreType.DMA((1,)),
            ],
            input_output_aliases=aliases,
            compiler_params=pltpu.CompilerParams(vmem_limit_bytes=40 * 1024 * 1024),
            cost_estimate=pl.CostEstimate(
                flops=60 * work, transcendentals=0, bytes_accessed=8 * work
            ),
        )(*operands)

    returned = lax.all_to_all(heat, "gy", split_axis=0, concat_axis=0, tiled=True)
    returned = returned.reshape(gy, levels, columns, LANES).transpose(1, 0, 2, 3)
    return out, warmed + returned.reshape(thermal_anomaly.shape)


def solution(mesh):
    return jax.shard_map(
        per_device,
        mesh=mesh,
        in_specs=(
            P(None, ("gx", "gy"), None, None),
            P(None, "gx", "gy"),
            P(None, "gx", "gy"),
            P(None, "gx", "gy"),
            P(None, "gx", "gy"),
            P("gx", "gy"),
            P(None, "gx", "gy"),
            P(("gx", "gy"), None),
            P(("gx", "gy"), None),
            P(),
            P(),
            P(),
            P(),
        ),
        out_specs=(P(None, ("gx", "gy"), None, None), P(None, "gx", "gy")),
        check_vma=False,
    )
```

```python
import functools

import jax
import jax.numpy as jnp
import numpy as np
from jax import lax
from jax.experimental import pallas as pl
from jax.experimental.pallas import tpu as pltpu
from jax.sharding import PartitionSpec as P


SUB = 3
NBIN = 8
NW = 4
SPREAD_FACTOR = 0.2

LANES = 128
MARGIN = 16
NEAR = 8
RIM = 2
CHUNKS = (2, 3, 2, 1)

UV_ROWS = 24
MOIST_ROW = 48
DEPTH_ROW = 64
SUN_ROW = 80
EDGE_ROW = 88
FIELD_ROWS = 96
PAIRS = 20


def spread_matrix():
    out = np.zeros((PAIRS, LANES, 2 * LANES), np.float32)
    for p in range(12):
        for part in range(3):
            out[p, 24 * part + p, :LANES] = 1.0
            out[p, 24 * part + 12 + p, LANES:] = 1.0
    for x in range(8):
        for part in range(3):
            out[12 + x, 72 + 8 * part + x, :LANES] = 1.0
        out[12 + x, 96 + x, LANES:] = 1.0
    return out


def three_parts(x):
    high = x.astype(jnp.bfloat16).astype(jnp.float32)
    rest = x - high
    middle = rest.astype(jnp.bfloat16).astype(jnp.float32)
    return [high, middle, rest - middle]


def chunk_rows(k):
    start = sum(CHUNKS[:k]) * LANES
    stop = start + CHUNKS[k] * LANES
    low = start - MARGIN if k == 0 else start + MARGIN
    return low, stop + (0 if k == len(CHUNKS) - 1 else MARGIN)


def slice_pieces(low, top):
    cuts = [low] + [c for c in range(-LANES, top, LANES) if low < c < top] + [top]
    return list(zip(cuts[:-1], cuts[1:]))


def slice_copies(chunks, place, tracer, outs, sems):
    mine = place[0]
    blocks = tracer.shape[2] // LANES
    columns = tracer.shape[1]
    copies = []
    for n, k in enumerate(chunks):
        low, top = chunk_rows(k)
        for side in range(2):
            target = lax.rem(mine + (1 if side == 0 else blocks - 1), blocks)
            first = columns - SUB if side == 0 else 0
            for a, b in slice_pieces(low, top):
                block = lax.rem(target + 1 + (a // LANES) + blocks, blocks)
                row = pl.multiple_of(block * LANES + a % LANES, MARGIN)
                copies.append(
                    pltpu.make_async_copy(
                        tracer.at[:, first : first + SUB, pl.ds(row, b - a), :],
                        outs[2 * n + side].at[:, :, a - low : b - low, :],
                        sems.at[len(copies)],
                    )
                )
    return copies


def copy_count(chunks):
    return sum(2 * len(slice_pieces(*chunk_rows(k))) for k in chunks)


def first_slice_kernel(place, tracer, u, v, warmth, up, down, rim_up, rim_down, sems):
    copies = slice_copies((0,), place, tracer, (up, down), sems)
    for copy in copies:
        copy.start()
    span = u.shape[1]
    for f in range(4):
        source = (u, v)[f // 2]
        rim_up[RIM * f : RIM * (f + 1), :] = source[f % 2, span - RIM : span, :]
        rim_down[RIM * f : RIM * (f + 1), :] = source[f % 2, 0:RIM, :]
    for level in range(2):
        at = 4 * RIM + level
        rim_up[at : at + 1, :] = warmth[level, span - 1 : span, :]
        rim_down[at : at + 1, :] = warmth[level, 0:1, :]
    at = 4 * RIM + 2
    rim_up[at:, :] = jnp.zeros((rim_up.shape[0] - at, LANES), jnp.float32)
    rim_down[at:, :] = jnp.zeros((rim_up.shape[0] - at, LANES), jnp.float32)
    for copy in copies:
        copy.wait()


def later_slice_kernel(place, tracer, *refs):
    outs, sems = refs[:-1], refs[-1]
    copies = slice_copies(tuple(range(1, len(CHUNKS))), place, tracer, outs, sems)
    for copy in copies:
        copy.start()
    for copy in copies:
        copy.wait()


def pack_kernel(place, u, v, moisture, depth, sun, warmth, low, high, out, ext):
    mine = place[0]
    parts = u.shape[1] // 8
    for f in range(4):
        source = (u, v)[f // 2]
        ext[f, 8 : 8 + u.shape[1], :] = source[f % 2]
        ext[f, 8 - RIM : 8, :] = low[RIM * f : RIM * (f + 1), :]
        ext[f, 8 + u.shape[1] : 8 + u.shape[1] + RIM, :] = high[RIM * f : RIM * (f + 1), :]
    turned = warmth[...].reshape(2 * u.shape[1], LANES).T
    last = turned[LANES - 1 :, :]
    initial = turned[:1, :]
    wide = 8 + 2 * RIM
    for d in range(parts):
        for level in range(2):
            base = UV_ROWS * level
            out[d, base : base + wide, :] = ext[level, 8 * d + 8 - RIM : 8 * d + 16 + RIM, :]
            out[d, base + wide : base + 2 * wide, :] = ext[
                2 + level, 8 * d + 8 - RIM : 8 * d + 16 + RIM, :
            ]
            out[d, MOIST_ROW + 8 * level : MOIST_ROW + 8 * level + 8, :] = moisture[
                level, 8 * d : 8 * d + 8, :
            ]
            out[d, DEPTH_ROW + 8 * level : DEPTH_ROW + 8 * level + 8, :] = depth[
                level, 8 * d : 8 * d + 8, :
            ]
        out[d, SUN_ROW : SUN_ROW + 8, :] = sun[8 * d : 8 * d + 8, :]
        row = jnp.where(mine + 1 == d, last, jnp.where(mine - 1 == d, initial, 0.0))
        out[d, EDGE_ROW : EDGE_ROW + 8, :] = jnp.broadcast_to(row, (8, LANES))


def turn_kernel(fields, kind, bins, turned, classes):
    for block in range(fields.shape[0]):
        lanes = slice(block * LANES, (block + 1) * LANES)
        classes[block] = bins[:, lanes]
        for level in range(2):
            parts = three_parts(fields[block, UV_ROWS * level : UV_ROWS * (level + 1), :])
            if level == 0:
                parts += three_parts(fields[block, DEPTH_ROW : DEPTH_ROW + 8, :])
                parts.append(kind[:, lanes].astype(jnp.float32))
                parts.append(jnp.zeros((24, LANES), jnp.float32))
            else:
                parts.append(jnp.zeros((56, LANES), jnp.float32))
            turned[level, block] = jnp.concatenate(parts, axis=0).T.astype(jnp.bfloat16)


def warm_kernel(place, warmth, low, high, fields, out, ext):
    mine = place[0]
    tiles = fields.shape[0]
    span = warmth.shape[1]
    lane = lax.broadcasted_iota(jnp.int32, (span, LANES), 1)
    left = fields[jnp.maximum(mine - 1, 0), EDGE_ROW : EDGE_ROW + 1, :]
    right = fields[jnp.minimum(mine + 1, tiles - 1), EDGE_ROW : EDGE_ROW + 1, :]
    at = 4 * RIM
    for level in range(2):
        here = warmth[level]
        ext[8 : 8 + span, :] = here
        ext[7:8, :] = low[at + level : at + level + 1, :]
        ext[8 + span : 9 + span, :] = high[at + level : at + level + 1, :]
        left_rows = jnp.broadcast_to(left[:, level * span : (level + 1) * span], (LANES, span)).T
        right_rows = jnp.broadcast_to(right[:, level * span : (level + 1) * span], (LANES, span)).T
        west = jnp.where(lane == 0, left_rows, pltpu.roll(here, 1, 1))
        east = jnp.where(lane == LANES - 1, right_rows, pltpu.roll(here, LANES - 1, 1))
        laplace = ext[9 : 9 + span, :] + ext[7 : 7 + span, :] + east + west - 4.0 * here
        out[level] = here + SPREAD_FACTOR * laplace


def row_blocks(first, count, size):
    return [(r, min(size, first + count - r)) for r in range(first, first + count, size)]


def chunk_kernel(k, *refs):
    first, final = k == 0, k == len(CHUNKS) - 1
    count = CHUNKS[k]
    refs = list(refs)
    place, sunlight, fields, classes, turned, spread, table, speeds, tracer = refs[:9]
    del refs[:9]
    west, east = refs[:2]
    del refs[:2]
    before = (None, None)
    if not first:
        before = refs[:2]
        del refs[:2]
        around = (None, None)
        if final:
            around = refs[:2]
            del refs[:2]
            del refs[:1]
        else:
            del refs[:2]
    out, heat = refs[:2]
    even, odd, coef, result, thick, warm, out_sems, heat_sems = refs[2:]

    columns = 8
    wide = columns + 2 * SUB
    mine, z = place[0], place[1]
    blocks = fields.shape[0]
    grid_rows = tracer.shape[2]
    top = MARGIN + LANES

    sublane = lax.broadcasted_iota(jnp.int32, (8, LANES), 0)
    weights = jnp.zeros((8, LANES), jnp.float32)
    for w in range(NW):
        weights = jnp.where(sublane == NW + w, sunlight[w], weights)
    lane = lax.broadcasted_iota(jnp.int32, (1, LANES), 1)
    category = jnp.where(lane < 72, lane % 24, -1).astype(jnp.float32)

    def wide_of(x):
        return x.astype(jnp.float32)

    def copies(j, slot, which=None):
        block = lax.rem(mine + 1 + sum(CHUNKS[:k]) + j, blocks)
        row = pl.multiple_of(block * LANES, LANES)
        these = []
        for level in (0, 1) if which is None else (which,):
            if level < 2:
                source, target = result.at[slot, level], out.at[level, :, pl.ds(row, LANES), :]
                these.append(pltpu.make_async_copy(source, target, out_sems.at[slot, level]))
        if which == 2 or (which is None and not final):
            these.append(pltpu.make_async_copy(warm.at[slot], heat.at[block], heat_sems.at[slot]))
        return these

    def step(source, c, i, r0, n):
        here = source[c, r0 : r0 + n, :]
        u = coef[2 * i, r0 - NEAR : r0 - NEAR + n, :]
        v = coef[2 * i + 1, r0 - NEAR : r0 - NEAR + n, :]
        across = jnp.where(u > 0.0, source[c - 1, r0 : r0 + n, :], source[c + 1, r0 : r0 + n, :])
        along = jnp.where(
            v > 0.0, source[c, pl.ds(z + (r0 - 1), n), :], source[c, pl.ds(z + (r0 + 1), n), :]
        )
        return here - jnp.abs(u) * (here - across) - jnp.abs(v) * (here - along)

    def one_block(j, carry):
        slot = lax.rem(j, 2)
        block = lax.rem(mine + 1 + sum(CHUNKS[:k]) + j, blocks)
        row = pl.multiple_of(block * LANES, LANES)
        low_row = pl.multiple_of(jnp.maximum(row - MARGIN, 0), MARGIN)
        high_row = pl.multiple_of(jnp.minimum(row + LANES, grid_rows - MARGIN), MARGIN)
        low_block = jnp.maximum(block - 1, 0)
        high_block = jnp.minimum(block + 1, blocks - 1)
        has_low = jnp.where(block != 0, 1.0, 0.0)
        has_high = jnp.where(block != blocks - 1, 1.0, 0.0)

        if count > 2:

            @pl.when(j >= 2)
            def _():
                for copy in copies(j - 2, slot):
                    copy.wait()

        for level in (1, 0):
            low_margin = wide_of(turned[level, low_block, LANES - MARGIN :, :]) * has_low
            high_margin = wide_of(turned[level, high_block, :MARGIN, :]) * has_high
            middle = turned[level, block]
            lhs = jnp.concatenate(
                [low_margin.astype(jnp.bfloat16), middle, high_margin.astype(jnp.bfloat16)], axis=0
            )

            def widen(at, low, head, tail, high):
                even[at, NEAR:MARGIN, :] = wide_of(low)[NEAR:, :] * has_low
                even[at, MARGIN : 2 * MARGIN, :] = wide_of(head)
                even[at, 2 * MARGIN : top, :] = wide_of(tail)
                even[at, top : top + NEAR, :] = wide_of(high)[:NEAR, :] * has_high

            for x in range(columns):
                widen(
                    SUB + x,
                    tracer[level, x, pl.ds(low_row, MARGIN), :],
                    tracer[level, x, pl.ds(row, MARGIN), :],
                    tracer[level, x, pl.ds(pl.multiple_of(row + MARGIN, MARGIN), LANES - MARGIN), :],
                    tracer[level, x, pl.ds(high_row, MARGIN), :],
                )

            def rims(at_start):
                for side, (rim, prior) in enumerate(zip((west, east), before)):
                    for c in range(SUB):
                        at = c + side * (SUB + columns)
                        if at_start:
                            end = prior.shape[2]
                            low = prior[level, c, end - 2 * MARGIN : end - MARGIN, :]
                            head = prior[level, c, end - MARGIN : end, :]
                            tail = rim[level, c, 0 : LANES - MARGIN, :]
                            if final:
                                high = around[side][level, c, MARGIN : 2 * MARGIN, :]
                            else:
                                high = rim[level, c, LANES - MARGIN : LANES, :]
                        else:
                            base = j * LANES + (0 if first else -2 * MARGIN)
                            low, head, tail, high = (
                                rim[level, c, pl.ds(pl.multiple_of(base + a, MARGIN), n), :]
                                for a, n in (
                                    (0, MARGIN),
                                    (MARGIN, MARGIN),
                                    (2 * MARGIN, LANES - MARGIN),
                                    (top, MARGIN),
                                )
                            )
                        widen(at, low, head, tail, high)

            if first:
                rims(False)
            elif count == 1:
                rims(True)
            else:
                pl.when(j == 0)(functools.partial(rims, True))
                pl.when(j != 0)(functools.partial(rims, False))

            for c in range(1, wide - 1):
                both = jnp.dot(lhs, spread[c - 1], preferred_element_type=jnp.float32)
                coef[2 * c - 2] = both[NEAR : top + NEAR, :LANES]
                coef[2 * c - 1] = both[NEAR : top + NEAR, LANES:]
                for r0, n in row_blocks(NEAR, LANES + 2 * NEAR, 72):
                    odd[c, r0 : r0 + n, :] = step(even, c, c - 1, r0, n)
            for c in range(2, wide - 2):
                for r0, n in row_blocks(NEAR, LANES + 2 * NEAR, 72):
                    even[c, r0 : r0 + n, :] = step(odd, c, c - 1, r0, n)

            for x in range(columns):
                c = x + SUB
                if level == 0:
                    pair = jnp.dot(middle, spread[12 + x], preferred_element_type=jnp.float32)
                    depth = pair[:, :LANES]
                    hot = jnp.where(pair[:, LANES:] == category, 1.0, 0.0).astype(jnp.bfloat16)
                    speed = jnp.dot(hot, speeds[...], preferred_element_type=jnp.float32)
                for r0, n in row_blocks(MARGIN, LANES, 64):
                    now = step(even, c, c - 1, r0, n)
                    if level == 0:
                        part = slice(r0 - MARGIN, r0 - MARGIN + n)
                        now = now * depth[part] / (depth[part] + speed[part])
                    result[slot, level, x, r0 - MARGIN : r0 - MARGIN + n, :] = now
                rounded = result[slot, level, x].astype(jnp.bfloat16)
                projected = lax.dot_general(
                    table[...], rounded, (((1,), (1,)), ((), ())), preferred_element_type=jnp.float32
                )
                which = classes[block, x : x + 1, :]
                dry = jnp.zeros((8, LANES), jnp.float32)
                wet = jnp.zeros((8, LANES), jnp.float32)
                for b in range(NBIN):
                    dry = jnp.where(which == b, projected[8 * b : 8 * b + 8], dry)
                    wet = jnp.where(which == b, projected[64 + 8 * b : 72 + 8 * b], wet)
                at = 8 * level + x
                moist = fields[block, MOIST_ROW + at : MOIST_ROW + at + 1, :]
                thickness = fields[block, DEPTH_ROW + at : DEPTH_ROW + at + 1, :]
                sun = fields[block, SUN_ROW + x : SUN_ROW + x + 1, :]
                growth = moist / (1.0 - moist)
                optical = (dry + growth * wet) * thickness
                if level == 1:
                    thick[x] = optical
                    lit = weights * optical
                else:
                    overhead = pltpu.roll(thick[x], NW, 0)
                    lit = weights * optical * jnp.exp(-overhead / sun)
                lit = sun * jnp.sum(lit, axis=0, keepdims=True)
                if final:
                    heat[at : at + 1, :] = lit
                else:
                    warm[slot, at : at + 1, :] = lit
            copies(j, slot, level)[0].start()
        if not final:
            copies(j, slot, 2)[0].start()
        return carry

    if count == 1:
        one_block(0, 0)
    else:
        lax.fori_loop(0, count, one_block, 0)
    for j in range(max(count - 2, 0), count):
        for copy in copies(j, j % 2):
            copy.wait()
    if first:
        copy = pltpu.make_async_copy(warm.at[0], heat.at[mine], heat_sems.at[0])
        copy.start()
        copy.wait()


def per_device(
    tracer_amounts,
    zonal_transit_ratio,
    meridional_transit_ratio,
    moisture_ratio,
    stratum_depths,
    sun_elevation_factor,
    thermal_anomaly,
    particle_class_map,
    ground_cover_kind,
    arid_extinction_table,
    swelling_factors,
    settling_velocities,
    arriving_irradiance,
):
    f32, bf16 = jnp.float32, jnp.bfloat16
    levels, columns, _, species = tracer_amounts.shape
    tile = thermal_anomaly.shape[1]
    gx, gy = lax.axis_size("gx"), lax.axis_size("gy")
    strips = ("gx", "gy")
    up = [(i, i + 1) for i in range(gx * gy - 1)]
    down = [(j, i) for i, j in up]
    gx_up = [(i, i + 1) for i in range(gx - 1)]
    gx_down = [(j, i) for i, j in gx_up]
    vmem = pl.BlockSpec(memory_space=pltpu.VMEM)
    smem = pl.BlockSpec(memory_space=pltpu.SMEM)
    hbm = pl.BlockSpec(memory_space=pltpu.HBM)

    mine = lax.axis_index("gy").astype(jnp.int32)
    place = jnp.stack([mine, jnp.zeros((), jnp.int32)])

    def halo_shape(k):
        low, high = chunk_rows(k)
        return jax.ShapeDtypeStruct((levels, SUB, high - low, species), bf16)

    rim_shape = jax.ShapeDtypeStruct((2 * 8, LANES), f32)
    *slices, rim_up, rim_down = pl.pallas_call(
        first_slice_kernel,
        out_shape=(halo_shape(0), halo_shape(0), rim_shape, rim_shape),
        in_specs=[smem, hbm] + [vmem] * 3,
        out_specs=(hbm, hbm, vmem, vmem),
        scratch_shapes=[pltpu.SemaphoreType.DMA((copy_count((0,)),))],
        compiler_params=pltpu.CompilerParams(vmem_limit_bytes=4 * 1024 * 1024),
        name="slice_first",
    )(place, tracer_amounts, zonal_transit_ratio, meridional_transit_ratio, thermal_anomaly)
    later = tuple(range(1, len(CHUNKS)))
    slices += pl.pallas_call(
        later_slice_kernel,
        out_shape=tuple(halo_shape(k) for k in later for _ in range(2)),
        in_specs=[smem, hbm],
        out_specs=(hbm,) * (2 * len(later)),
        scratch_shapes=[pltpu.SemaphoreType.DMA((copy_count(later),))],
        compiler_params=pltpu.CompilerParams(vmem_limit_bytes=4 * 1024 * 1024),
        name="slice_later",
    )(place, tracer_amounts)

    from_low = lax.ppermute(rim_up, "gx", gx_up)
    from_high = lax.ppermute(rim_down, "gx", gx_down)
    wests, easts = [], []
    for k in range(len(CHUNKS)):
        wests.append(lax.ppermute(slices[2 * k], strips, up))
        easts.append(lax.ppermute(slices[2 * k + 1], strips, down))

    packed = pl.pallas_call(
        pack_kernel,
        out_shape=jax.ShapeDtypeStruct((gy, FIELD_ROWS, LANES), f32),
        in_specs=[smem] + [vmem] * 8,
        out_specs=vmem,
        scratch_shapes=[pltpu.VMEM((4, tile + 16, LANES), f32)],
        compiler_params=pltpu.CompilerParams(vmem_limit_bytes=4 * 1024 * 1024),
        name="pack",
    )(
        place,
        zonal_transit_ratio,
        meridional_transit_ratio,
        moisture_ratio,
        stratum_depths,
        sun_elevation_factor,
        thermal_anomaly,
        from_low,
        from_high,
    )
    fields = lax.all_to_all(packed, "gy", split_axis=0, concat_axis=0, tiled=True)

    turned, classes = pl.pallas_call(
        turn_kernel,
        out_shape=(
            jax.ShapeDtypeStruct((levels, gy, LANES, LANES), bf16),
            jax.ShapeDtypeStruct((gy, columns, LANES), jnp.int32),
        ),
        in_specs=[vmem] * 3,
        out_specs=(vmem, vmem),
        compiler_params=pltpu.CompilerParams(vmem_limit_bytes=4 * 1024 * 1024),
        name="turn",
    )(fields, ground_cover_kind, particle_class_map)

    warmed = pl.pallas_call(
        warm_kernel,
        out_shape=jax.ShapeDtypeStruct(thermal_anomaly.shape, f32),
        in_specs=[smem] + [vmem] * 4,
        out_specs=vmem,
        scratch_shapes=[pltpu.VMEM((tile + 16, LANES), f32)],
        compiler_params=pltpu.CompilerParams(vmem_limit_bytes=4 * 1024 * 1024),
        name="warm",
    )(place, thermal_anomaly, from_low, from_high, fields)

    spread = jnp.asarray(spread_matrix(), bf16)
    table = jnp.concatenate([arid_extinction_table, swelling_factors], axis=1).T
    parts, rest = [], settling_velocities
    for _ in range(3):
        part = lax.reduce_precision(rest, 8, 7)
        parts.append(part.astype(bf16))
        rest = rest - part
    parts.append(jnp.zeros((LANES - 3 * settling_velocities.shape[0], species), bf16))
    speeds = jnp.concatenate(parts, axis=0)

    def run_chunk(k, out, heat):
        first, final = k == 0, k == len(CHUNKS) - 1
        operands = [
            place,
            arriving_irradiance,
            fields,
            classes,
            turned,
            spread,
            table,
            speeds,
            tracer_amounts,
            wests[k],
            easts[k],
        ]
        specs = [smem, smem] + [vmem] * 9
        heat_block = (levels * columns, LANES)
        out_shapes = [jax.ShapeDtypeStruct(tracer_amounts.shape, f32)]
        out_specs = [hbm]
        aliases = {}
        if not first:
            operands += [wests[k - 1], easts[k - 1]]
            specs += [vmem] * 2
            if final:
                operands += [wests[0], easts[0]]
                specs += [vmem] * 2
            aliases[len(operands)] = 0
            operands.append(out)
            specs.append(hbm)
        if final:
            out_shapes.append(jax.ShapeDtypeStruct(heat_block, f32))
            out_specs.append(vmem)
        else:
            if not first:
                aliases[len(operands)] = 1
                operands.append(heat)
                specs.append(hbm)
            out_shapes.append(jax.ShapeDtypeStruct((gy,) + heat_block, f32))
            out_specs.append(hbm)
        work = CHUNKS[k] * LANES * columns * levels * species
        span = LANES + 2 * MARGIN
        return pl.pallas_call(
            functools.partial(chunk_kernel, k),
            out_shape=tuple(out_shapes),
            in_specs=specs,
            out_specs=tuple(out_specs),
            scratch_shapes=[
                pltpu.VMEM((columns + 2 * SUB, span, LANES), f32),
                pltpu.VMEM((columns + 2 * SUB, span, LANES), f32),
                pltpu.VMEM((24, LANES + 2 * NEAR, LANES), f32),
                pltpu.VMEM((2, levels, columns, LANES, LANES), f32),
                pltpu.VMEM((columns, 8, LANES), f32),
                pltpu.VMEM((2, levels * columns, LANES), f32),
                pltpu.SemaphoreType.DMA((2, levels)),
                pltpu.SemaphoreType.DMA((2,)),
            ],
            input_output_aliases=aliases,
            compiler_params=pltpu.CompilerParams(vmem_limit_bytes=12 * 1024 * 1024),
            cost_estimate=pl.CostEstimate(
                flops=60 * work, transcendentals=0, bytes_accessed=8 * work
            ),
        )(*operands)

    out = heat = None
    for k in range(len(CHUNKS) - 1):
        out, heat = run_chunk(k, out, heat)
    returned = lax.all_to_all(heat, "gy", split_axis=0, concat_axis=0, tiled=True)
    out, own = run_chunk(len(CHUNKS) - 1, out, None)

    is_own = lax.broadcasted_iota(jnp.int32, (gy, 1, 1), 0) == mine
    returned = jnp.where(is_own, own[None], returned)
    returned = returned.reshape(gy, levels, columns, LANES).transpose(1, 0, 2, 3)
    return out, warmed + returned.reshape(thermal_anomaly.shape)


def solution(mesh):
    return jax.shard_map(
        per_device,
        mesh=mesh,
        in_specs=(
            P(None, ("gx", "gy"), None, None),
            P(None, "gx", "gy"),
            P(None, "gx", "gy"),
            P(None, "gx", "gy"),
            P(None, "gx", "gy"),
            P("gx", "gy"),
            P(None, "gx", "gy"),
            P(("gx", "gy"), None),
            P(("gx", "gy"), None),
            P(),
            P(),
            P(),
            P(),
        ),
        out_specs=(P(None, ("gx", "gy"), None, None), P(None, "gx", "gy")),
        check_vma=False,
    )
```

```python
import functools

import jax
import jax.numpy as jnp
import numpy as np
from jax import lax
from jax.experimental import pallas as pl
from jax.experimental.pallas import tpu as pltpu
from jax.sharding import PartitionSpec as P


SUB = 3
NBIN = 8
NW = 4
SPREAD_FACTOR = 0.2

LANES = 128
MARGIN = 16
NEAR = 8
RIM = 2
CHUNKS = (2, 3, 2, 1)

UV_ROWS = 24
MOIST_ROW = 48
DEPTH_ROW = 64
SUN_ROW = 80
EDGE_ROW = 88
FIELD_ROWS = 96
PAIRS = 20


def spread_matrix():
    out = np.zeros((PAIRS, LANES, 2 * LANES), np.float32)
    for p in range(12):
        for part in range(3):
            out[p, 24 * part + p, :LANES] = 1.0
            out[p, 24 * part + 12 + p, LANES:] = 1.0
    for x in range(8):
        for part in range(3):
            out[12 + x, 72 + 8 * part + x, :LANES] = 1.0
        out[12 + x, 96 + x, LANES:] = 1.0
    return out


def three_parts(x):
    high = x.astype(jnp.bfloat16).astype(jnp.float32)
    rest = x - high
    middle = rest.astype(jnp.bfloat16).astype(jnp.float32)
    return [high, middle, rest - middle]


def chunk_rows(k):
    start = sum(CHUNKS[:k]) * LANES
    stop = start + CHUNKS[k] * LANES
    low = start - MARGIN if k == 0 else start + MARGIN
    return low, stop + (0 if k == len(CHUNKS) - 1 else MARGIN)


def slice_pieces(low, top):
    cuts = [low] + [c for c in range(-LANES, top, LANES) if low < c < top] + [top]
    return list(zip(cuts[:-1], cuts[1:]))


def slice_copies(chunks, place, tracer, outs, sems):
    mine = place[0]
    odd = lax.rem(mine, 2)
    blocks = tracer.shape[2] // LANES
    columns = tracer.shape[1]
    copies = []
    for n, k in enumerate(chunks):
        low, top = chunk_rows(k)
        for swap in range(2):
            upward = odd if swap else 1 - odd
            target = lax.rem(mine + 2 * upward - 1 + blocks, blocks)
            first = upward * (columns - SUB)
            for a, b in slice_pieces(low, top):
                block = lax.rem(target + 1 + (a // LANES) + blocks, blocks)
                row = pl.multiple_of(block * LANES + a % LANES, MARGIN)
                copies.append(
                    pltpu.make_async_copy(
                        tracer.at[:, pl.ds(first, SUB), pl.ds(row, b - a), :],
                        outs[2 * n + swap].at[:, :, a - low : b - low, :],
                        sems.at[len(copies)],
                    )
                )
    return copies


def copy_count(chunks):
    return sum(2 * len(slice_pieces(*chunk_rows(k))) for k in chunks)


def first_slice_kernel(place, tracer, u, v, warmth, out_0, out_1, rim_0, rim_1, sems):
    copies = slice_copies((0,), place, tracer, (out_0, out_1), sems)
    for copy in copies:
        copy.start()
    span = u.shape[1]
    odd = place[2] == 1

    def put(at, low, high):
        n = low.shape[0]
        rim_0[at : at + n, :] = jnp.where(odd, low, high)
        rim_1[at : at + n, :] = jnp.where(odd, high, low)

    for f in range(4):
        source = (u, v)[f // 2]
        put(RIM * f, source[f % 2, 0:RIM, :], source[f % 2, span - RIM : span, :])
    for level in range(2):
        put(4 * RIM + level, warmth[level, 0:1, :], warmth[level, span - 1 : span, :])
    at = 4 * RIM + 2
    for rim in (rim_0, rim_1):
        rim[at:, :] = jnp.zeros((rim.shape[0] - at, LANES), jnp.float32)
    for copy in copies:
        copy.wait()


def later_slice_kernel(place, tracer, *refs):
    outs, sems = refs[:-1], refs[-1]
    copies = slice_copies(tuple(range(1, len(CHUNKS))), place, tracer, outs, sems)
    for copy in copies:
        copy.start()
    for copy in copies:
        copy.wait()


def rims_of(place, rim_0, rim_1):
    odd = place[2] == 1
    return jnp.where(odd, rim_0[...], rim_1[...]), jnp.where(odd, rim_1[...], rim_0[...])


def pack_kernel(place, u, v, moisture, depth, sun, warmth, rim_0, rim_1, out, ext):
    mine = place[0]
    low, high = rims_of(place, rim_0, rim_1)
    parts = u.shape[1] // 8
    for f in range(4):
        source = (u, v)[f // 2]
        ext[f, 8 : 8 + u.shape[1], :] = source[f % 2]
        ext[f, 8 - RIM : 8, :] = low[RIM * f : RIM * (f + 1), :]
        ext[f, 8 + u.shape[1] : 8 + u.shape[1] + RIM, :] = high[RIM * f : RIM * (f + 1), :]
    turned = warmth[...].reshape(2 * u.shape[1], LANES).T
    last = turned[LANES - 1 :, :]
    initial = turned[:1, :]
    wide = 8 + 2 * RIM
    for d in range(parts):
        for level in range(2):
            base = UV_ROWS * level
            out[d, base : base + wide, :] = ext[level, 8 * d + 8 - RIM : 8 * d + 16 + RIM, :]
            out[d, base + wide : base + 2 * wide, :] = ext[
                2 + level, 8 * d + 8 - RIM : 8 * d + 16 + RIM, :
            ]
            out[d, MOIST_ROW + 8 * level : MOIST_ROW + 8 * level + 8, :] = moisture[
                level, 8 * d : 8 * d + 8, :
            ]
            out[d, DEPTH_ROW + 8 * level : DEPTH_ROW + 8 * level + 8, :] = depth[
                level, 8 * d : 8 * d + 8, :
            ]
        out[d, SUN_ROW : SUN_ROW + 8, :] = sun[8 * d : 8 * d + 8, :]
        row = jnp.where(mine + 1 == d, last, jnp.where(mine - 1 == d, initial, 0.0))
        out[d, EDGE_ROW : EDGE_ROW + 8, :] = jnp.broadcast_to(row, (8, LANES))


def turn_kernel(fields, kind, bins, turned, classes):
    for block in range(fields.shape[0]):
        lanes = slice(block * LANES, (block + 1) * LANES)
        classes[block] = bins[:, lanes]
        for level in range(2):
            parts = three_parts(fields[block, UV_ROWS * level : UV_ROWS * (level + 1), :])
            if level == 0:
                parts += three_parts(fields[block, DEPTH_ROW : DEPTH_ROW + 8, :])
                parts.append(kind[:, lanes].astype(jnp.float32))
                parts.append(jnp.zeros((24, LANES), jnp.float32))
            else:
                parts.append(jnp.zeros((56, LANES), jnp.float32))
            turned[level, block] = jnp.concatenate(parts, axis=0).T.astype(jnp.bfloat16)


def warm_kernel(place, warmth, rim_0, rim_1, fields, out, ext):
    mine = place[0]
    low, high = rims_of(place, rim_0, rim_1)
    tiles = fields.shape[0]
    span = warmth.shape[1]
    lane = lax.broadcasted_iota(jnp.int32, (span, LANES), 1)
    left = fields[jnp.maximum(mine - 1, 0), EDGE_ROW : EDGE_ROW + 1, :]
    right = fields[jnp.minimum(mine + 1, tiles - 1), EDGE_ROW : EDGE_ROW + 1, :]
    at = 4 * RIM
    for level in range(2):
        here = warmth[level]
        ext[8 : 8 + span, :] = here
        ext[7:8, :] = low[at + level : at + level + 1, :]
        ext[8 + span : 9 + span, :] = high[at + level : at + level + 1, :]
        left_rows = jnp.broadcast_to(left[:, level * span : (level + 1) * span], (LANES, span)).T
        right_rows = jnp.broadcast_to(right[:, level * span : (level + 1) * span], (LANES, span)).T
        west = jnp.where(lane == 0, left_rows, pltpu.roll(here, 1, 1))
        east = jnp.where(lane == LANES - 1, right_rows, pltpu.roll(here, LANES - 1, 1))
        laplace = ext[9 : 9 + span, :] + ext[7 : 7 + span, :] + east + west - 4.0 * here
        out[level] = here + SPREAD_FACTOR * laplace


def own_kernel(place, tracer, fields, classes, turned, window, own_fields, own_classes, lhs, sems):
    mine = place[0]
    blocks = fields.shape[0]
    row = pl.multiple_of(mine * LANES, LANES)
    low = pl.multiple_of(jnp.maximum(row - MARGIN, 0), MARGIN)
    high = pl.multiple_of(jnp.minimum(row + LANES, tracer.shape[2] - MARGIN), MARGIN)
    copies = []
    for source, at, n in ((low, 0, MARGIN), (row, MARGIN, LANES), (high, MARGIN + LANES, MARGIN)):
        copies.append(
            pltpu.make_async_copy(
                tracer.at[:, :, pl.ds(source, n), :],
                window.at[:, :, at : at + n, :],
                sems.at[len(copies)],
            )
        )
    for copy in copies:
        copy.start()
    own_fields[...] = fields[mine]
    own_classes[...] = classes[mine]
    for level in range(2):
        lhs[level] = block_lhs(turned, level, mine, blocks)
    for copy in copies:
        copy.wait()


def block_lhs(turned, level, block, blocks):
    low = turned[level, jnp.maximum(block - 1, 0), LANES - MARGIN :, :].astype(jnp.float32)
    high = turned[level, jnp.minimum(block + 1, blocks - 1), :MARGIN, :].astype(jnp.float32)
    low = low * jnp.where(block != 0, 1.0, 0.0)
    high = high * jnp.where(block != blocks - 1, 1.0, 0.0)
    ends = [low.astype(jnp.bfloat16), high.astype(jnp.bfloat16)]
    return jnp.concatenate([ends[0], turned[level, block], ends[1]], axis=0)


def row_blocks(first, count, size):
    return [(r, min(size, first + count - r)) for r in range(first, first + count, size)]


def chunk_kernel(k, *refs):
    first, final = k == 0, k == len(CHUNKS) - 1
    count = CHUNKS[k]
    refs = list(refs)
    place, sunlight, spread, table, speeds, fields, classes, turned, tracer = refs[:9]
    del refs[:9]
    halos = refs[:2]
    del refs[:2]
    before = (None, None)
    if not first:
        before = refs[:2]
        del refs[:2]
        around = (None, None)
        if final:
            around = refs[:2]
            del refs[:2]
            del refs[:1]
        else:
            del refs[:2]
    out, heat = refs[:2]
    even, odd, coef, result, thick, warm, out_sems, heat_sems = refs[2:]

    columns = 8
    wide = columns + 2 * SUB
    mine, z = place[0], place[1]
    parity = lax.rem(mine, 2)
    blocks = out.shape[2] // LANES
    grid_rows = out.shape[2]
    top = MARGIN + LANES

    sublane = lax.broadcasted_iota(jnp.int32, (8, LANES), 0)
    weights = jnp.zeros((8, LANES), jnp.float32)
    for w in range(NW):
        weights = jnp.where(sublane == NW + w, sunlight[w], weights)
    lane = lax.broadcasted_iota(jnp.int32, (1, LANES), 1)
    category = jnp.where(lane < 72, lane % 24, -1).astype(jnp.float32)

    def wide_of(x):
        return x.astype(jnp.float32)

    def copies(j, slot, which=None):
        block = lax.rem(mine + 1 + sum(CHUNKS[:k]) + j, blocks)
        row = pl.multiple_of(block * LANES, LANES)
        these = []
        for level in (0, 1) if which is None else (which,):
            if level < 2:
                source, target = result.at[slot, level], out.at[level, :, pl.ds(row, LANES), :]
                these.append(pltpu.make_async_copy(source, target, out_sems.at[slot, level]))
        if which == 2 or (which is None and not final):
            these.append(pltpu.make_async_copy(warm.at[slot], heat.at[block], heat_sems.at[slot]))
        return these

    def field_row(block, at):
        return fields[at : at + 1, :] if final else fields[block, at : at + 1, :]

    def step(source, c, i, r0, n):
        here = source[c, r0 : r0 + n, :]
        u = coef[2 * i, r0 - NEAR : r0 - NEAR + n, :]
        v = coef[2 * i + 1, r0 - NEAR : r0 - NEAR + n, :]
        across = jnp.where(u > 0.0, source[c - 1, r0 : r0 + n, :], source[c + 1, r0 : r0 + n, :])
        along = jnp.where(
            v > 0.0, source[c, pl.ds(z + (r0 - 1), n), :], source[c, pl.ds(z + (r0 + 1), n), :]
        )
        return here - jnp.abs(u) * (here - across) - jnp.abs(v) * (here - along)

    def one_block(j, carry):
        slot = lax.rem(j, 2)
        block = lax.rem(mine + 1 + sum(CHUNKS[:k]) + j, blocks)
        row = pl.multiple_of(block * LANES, LANES)
        low_row = pl.multiple_of(jnp.maximum(row - MARGIN, 0), MARGIN)
        high_row = pl.multiple_of(jnp.minimum(row + LANES, grid_rows - MARGIN), MARGIN)
        has_low = jnp.where(block != 0, 1.0, 0.0)
        has_high = jnp.where(block != blocks - 1, 1.0, 0.0)

        if count > 2:

            @pl.when(j >= 2)
            def _():
                for copy in copies(j - 2, slot):
                    copy.wait()

        for level in (1, 0):
            lhs = turned[level] if final else block_lhs(turned, level, block, blocks)
            for c in range(wide - 2):
                both = jnp.dot(lhs, spread[c], preferred_element_type=jnp.float32)
                coef[2 * c] = both[NEAR : top + NEAR, :LANES]
                coef[2 * c + 1] = both[NEAR : top + NEAR, LANES:]

            def widen(at, low, head, tail, high):
                even[at, NEAR:MARGIN, :] = wide_of(low)[NEAR:, :] * has_low
                even[at, MARGIN : 2 * MARGIN, :] = wide_of(head)
                even[at, 2 * MARGIN : top, :] = wide_of(tail)
                even[at, top : top + NEAR, :] = wide_of(high)[:NEAR, :] * has_high

            def widen_column(x, carry):
                if final:
                    parts = [
                        tracer[level, x, r : r + n, :]
                        for r, n in (
                            (0, MARGIN),
                            (MARGIN, MARGIN),
                            (2 * MARGIN, LANES - MARGIN),
                            (top, MARGIN),
                        )
                    ]
                else:
                    inner = pl.multiple_of(row + MARGIN, MARGIN)
                    parts = [
                        tracer[level, x, pl.ds(low_row, MARGIN), :],
                        tracer[level, x, pl.ds(row, MARGIN), :],
                        tracer[level, x, pl.ds(inner, LANES - MARGIN), :],
                        tracer[level, x, pl.ds(high_row, MARGIN), :],
                    ]
                widen(SUB + x, *parts)
                return carry

            lax.fori_loop(0, columns, widen_column, 0)

            def rims(at_start):
                for swap, (rim, prior) in enumerate(zip(halos, before)):
                    for c in range(SUB):
                        at = c + (parity if swap else 1 - parity) * (SUB + columns)
                        if at_start:
                            end = prior.shape[2]
                            low = prior[level, c, end - 2 * MARGIN : end - MARGIN, :]
                            head = prior[level, c, end - MARGIN : end, :]
                            tail = rim[level, c, 0 : LANES - MARGIN, :]
                            if final:
                                high = around[swap][level, c, MARGIN : 2 * MARGIN, :]
                            else:
                                high = rim[level, c, LANES - MARGIN : LANES, :]
                        else:
                            base = j * LANES + (0 if first else -2 * MARGIN)
                            low, head, tail, high = (
                                rim[level, c, pl.ds(pl.multiple_of(base + a, MARGIN), n), :]
                                for a, n in (
                                    (0, MARGIN),
                                    (MARGIN, MARGIN),
                                    (2 * MARGIN, LANES - MARGIN),
                                    (top, MARGIN),
                                )
                            )
                        widen(at, low, head, tail, high)

            if first:
                rims(False)
            elif count == 1:
                rims(True)
            else:
                pl.when(j == 0)(functools.partial(rims, True))
                pl.when(j != 0)(functools.partial(rims, False))

            def substep_one(c, carry):
                for r0, n in row_blocks(NEAR, LANES + 2 * NEAR, 72):
                    odd[c, r0 : r0 + n, :] = step(even, c, c - 1, r0, n)
                return carry

            def substep_two(c, carry):
                for r0, n in row_blocks(NEAR, LANES + 2 * NEAR, 72):
                    even[c, r0 : r0 + n, :] = step(odd, c, c - 1, r0, n)
                return carry

            lax.fori_loop(1, wide - 1, substep_one, 0)
            lax.fori_loop(2, wide - 2, substep_two, 0)

            for x in range(columns):
                c = x + SUB
                if level == 0:
                    pair = jnp.dot(lhs[MARGIN:top], spread[12 + x], preferred_element_type=jnp.float32)
                    depth = pair[:, :LANES]
                    hot = jnp.where(pair[:, LANES:] == category, 1.0, 0.0).astype(jnp.bfloat16)
                    speed = jnp.dot(hot, speeds[...], preferred_element_type=jnp.float32)
                for r0, n in row_blocks(MARGIN, LANES, 64):
                    now = step(even, c, c - 1, r0, n)
                    if level == 0:
                        part = slice(r0 - MARGIN, r0 - MARGIN + n)
                        now = now * depth[part] / (depth[part] + speed[part])
                    result[slot, level, x, r0 - MARGIN : r0 - MARGIN + n, :] = now
                rounded = result[slot, level, x].astype(jnp.bfloat16)
                projected = lax.dot_general(
                    table[...], rounded, (((1,), (1,)), ((), ())), preferred_element_type=jnp.float32
                )
                which = classes[x : x + 1, :] if final else classes[block, x : x + 1, :]
                dry = jnp.zeros((8, LANES), jnp.float32)
                wet = jnp.zeros((8, LANES), jnp.float32)
                for b in range(NBIN):
                    dry = jnp.where(which == b, projected[8 * b : 8 * b + 8], dry)
                    wet = jnp.where(which == b, projected[64 + 8 * b : 72 + 8 * b], wet)
                at = 8 * level + x
                moist = field_row(block, MOIST_ROW + at)
                thickness = field_row(block, DEPTH_ROW + at)
                sun = field_row(block, SUN_ROW + x)
                growth = moist / (1.0 - moist)
                optical = (dry + growth * wet) * thickness
                if level == 1:
                    thick[x] = optical
                    lit = weights * optical
                else:
                    overhead = pltpu.roll(thick[x], NW, 0)
                    lit = weights * optical * jnp.exp(-overhead / sun)
                lit = sun * jnp.sum(lit, axis=0, keepdims=True)
                if final:
                    heat[at : at + 1, :] = lit
                else:
                    warm[slot, at : at + 1, :] = lit
            copies(j, slot, level)[0].start()
        if not final:
            copies(j, slot, 2)[0].start()
        return carry

    if count == 1:
        one_block(0, 0)
    else:
        lax.fori_loop(0, count, one_block, 0)
    for j in range(max(count - 2, 0), count):
        for copy in copies(j, j % 2):
            copy.wait()
    if first:
        copy = pltpu.make_async_copy(warm.at[0], heat.at[mine], heat_sems.at[0])
        copy.start()
        copy.wait()


def per_device(
    tracer_amounts,
    zonal_transit_ratio,
    meridional_transit_ratio,
    moisture_ratio,
    stratum_depths,
    sun_elevation_factor,
    thermal_anomaly,
    particle_class_map,
    ground_cover_kind,
    arid_extinction_table,
    swelling_factors,
    settling_velocities,
    arriving_irradiance,
):
    f32, bf16 = jnp.float32, jnp.bfloat16
    levels, columns, _, species = tracer_amounts.shape
    tile = thermal_anomaly.shape[1]
    gx, gy = lax.axis_size("gx"), lax.axis_size("gy")
    strips = ("gx", "gy")

    def swaps(n):
        pairs = [[(i, i + 1) for i in range(start, n - 1, 2)] for start in (0, 1)]
        return [p + [(j, i) for i, j in p] for p in pairs]

    vmem = pl.BlockSpec(memory_space=pltpu.VMEM)
    smem = pl.BlockSpec(memory_space=pltpu.SMEM)
    hbm = pl.BlockSpec(memory_space=pltpu.HBM)

    mine = lax.axis_index("gy").astype(jnp.int32)
    gx_odd = lax.rem(lax.axis_index("gx").astype(jnp.int32), 2)
    place = jnp.stack([mine, jnp.zeros((), jnp.int32), gx_odd])

    def halo_shape(k):
        low, high = chunk_rows(k)
        return jax.ShapeDtypeStruct((levels, SUB, high - low, species), bf16)

    rim_shape = jax.ShapeDtypeStruct((2 * 8, LANES), f32)
    *slices, rim_0, rim_1 = pl.pallas_call(
        first_slice_kernel,
        out_shape=(halo_shape(0), halo_shape(0), rim_shape, rim_shape),
        in_specs=[smem, hbm] + [vmem] * 3,
        out_specs=(hbm, hbm, vmem, vmem),
        scratch_shapes=[pltpu.SemaphoreType.DMA((copy_count((0,)),))],
        compiler_params=pltpu.CompilerParams(vmem_limit_bytes=4 * 1024 * 1024),
        name="slice_first",
    )(place, tracer_amounts, zonal_transit_ratio, meridional_transit_ratio, thermal_anomaly)
    later = tuple(range(1, len(CHUNKS)))
    slices += pl.pallas_call(
        later_slice_kernel,
        out_shape=tuple(halo_shape(k) for k in later for _ in range(2)),
        in_specs=[smem, hbm],
        out_specs=(hbm,) * (2 * len(later)),
        scratch_shapes=[pltpu.SemaphoreType.DMA((copy_count(later),))],
        compiler_params=pltpu.CompilerParams(vmem_limit_bytes=4 * 1024 * 1024),
        name="slice_later",
    )(place, tracer_amounts)

    rims = [lax.ppermute(r, "gx", p) for r, p in zip((rim_0, rim_1), swaps(gx))]
    halos = []
    for k in range(len(CHUNKS)):
        pair = slices[2 * k : 2 * k + 2]
        halos.append([lax.ppermute(h, strips, p) for h, p in zip(pair, swaps(gx * gy))])

    packed = pl.pallas_call(
        pack_kernel,
        out_shape=jax.ShapeDtypeStruct((gy, FIELD_ROWS, LANES), f32),
        in_specs=[smem] + [vmem] * 8,
        out_specs=vmem,
        scratch_shapes=[pltpu.VMEM((4, tile + 16, LANES), f32)],
        compiler_params=pltpu.CompilerParams(vmem_limit_bytes=4 * 1024 * 1024),
        name="pack",
    )(
        place,
        zonal_transit_ratio,
        meridional_transit_ratio,
        moisture_ratio,
        stratum_depths,
        sun_elevation_factor,
        thermal_anomaly,
        *rims,
    )
    fields = lax.all_to_all(packed, "gy", split_axis=0, concat_axis=0, tiled=True)

    turned, classes = pl.pallas_call(
        turn_kernel,
        out_shape=(
            jax.ShapeDtypeStruct((levels, gy, LANES, LANES), bf16),
            jax.ShapeDtypeStruct((gy, columns, LANES), jnp.int32),
        ),
        in_specs=[vmem] * 3,
        out_specs=(vmem, vmem),
        compiler_params=pltpu.CompilerParams(vmem_limit_bytes=4 * 1024 * 1024),
        name="turn",
    )(fields, ground_cover_kind, particle_class_map)

    warmed = pl.pallas_call(
        warm_kernel,
        out_shape=jax.ShapeDtypeStruct(thermal_anomaly.shape, f32),
        in_specs=[smem] + [vmem] * 4,
        out_specs=vmem,
        scratch_shapes=[pltpu.VMEM((tile + 16, LANES), f32)],
        compiler_params=pltpu.CompilerParams(vmem_limit_bytes=4 * 1024 * 1024),
        name="warm",
    )(place, thermal_anomaly, *rims, fields)

    whole = pl.pallas_call(
        own_kernel,
        out_shape=(
            jax.ShapeDtypeStruct((levels, columns, LANES + 2 * MARGIN, species), bf16),
            jax.ShapeDtypeStruct((FIELD_ROWS, LANES), f32),
            jax.ShapeDtypeStruct((columns, LANES), jnp.int32),
            jax.ShapeDtypeStruct((levels, LANES + 2 * MARGIN, LANES), bf16),
        ),
        in_specs=[smem, hbm] + [vmem] * 3,
        out_specs=(vmem,) * 4,
        scratch_shapes=[pltpu.SemaphoreType.DMA((3,))],
        compiler_params=pltpu.CompilerParams(vmem_limit_bytes=4 * 1024 * 1024),
        name="own",
    )(place, tracer_amounts, fields, classes, turned)
    own_inputs = [whole[1], whole[2], whole[3], whole[0]]

    spread = jnp.asarray(spread_matrix(), bf16)
    table = jnp.concatenate([arid_extinction_table, swelling_factors], axis=1).T
    parts, rest = [], settling_velocities
    for _ in range(3):
        part = lax.reduce_precision(rest, 8, 7)
        parts.append(part.astype(bf16))
        rest = rest - part
    parts.append(jnp.zeros((LANES - 3 * settling_velocities.shape[0], species), bf16))
    speeds = jnp.concatenate(parts, axis=0)

    def run_chunk(k, out, heat):
        first, final = k == 0, k == len(CHUNKS) - 1
        operands = [place, arriving_irradiance, spread, table, speeds]
        operands += own_inputs if final else [fields, classes, turned, tracer_amounts]
        operands += halos[k]
        specs = [smem, smem] + [vmem] * 9
        heat_block = (levels * columns, LANES)
        out_shapes = [jax.ShapeDtypeStruct(tracer_amounts.shape, f32)]
        out_specs = [hbm]
        aliases = {}
        if not first:
            operands += halos[k - 1]
            specs += [vmem] * 2
            if final:
                operands += halos[0]
                specs += [vmem] * 2
            aliases[len(operands)] = 0
            operands.append(out)
            specs.append(hbm)
        if final:
            out_shapes.append(jax.ShapeDtypeStruct(heat_block, f32))
            out_specs.append(vmem)
        else:
            if not first:
                aliases[len(operands)] = 1
                operands.append(heat)
                specs.append(hbm)
            out_shapes.append(jax.ShapeDtypeStruct((gy,) + heat_block, f32))
            out_specs.append(hbm)
        work = CHUNKS[k] * LANES * columns * levels * species
        span = LANES + 2 * MARGIN
        return pl.pallas_call(
            functools.partial(chunk_kernel, k),
            out_shape=tuple(out_shapes),
            in_specs=specs,
            out_specs=tuple(out_specs),
            scratch_shapes=[
                pltpu.VMEM((columns + 2 * SUB, span, LANES), f32),
                pltpu.VMEM((columns + 2 * SUB, span, LANES), f32),
                pltpu.VMEM((24, LANES + 2 * NEAR, LANES), f32),
                pltpu.VMEM((2, levels, columns, LANES, LANES), f32),
                pltpu.VMEM((columns, 8, LANES), f32),
                pltpu.VMEM((2, levels * columns, LANES), f32),
                pltpu.SemaphoreType.DMA((2, levels)),
                pltpu.SemaphoreType.DMA((2,)),
            ],
            input_output_aliases=aliases,
            compiler_params=pltpu.CompilerParams(vmem_limit_bytes=12 * 1024 * 1024),
            cost_estimate=pl.CostEstimate(
                flops=60 * work, transcendentals=0, bytes_accessed=8 * work
            ),
        )(*operands)

    out = heat = None
    for k in range(len(CHUNKS) - 1):
        out, heat = run_chunk(k, out, heat)
    returned = lax.all_to_all(heat, "gy", split_axis=0, concat_axis=0, tiled=True)
    out, own = run_chunk(len(CHUNKS) - 1, out, None)

    is_own = lax.broadcasted_iota(jnp.int32, (gy, 1, 1), 0) == mine
    returned = jnp.where(is_own, own[None], returned)
    returned = returned.reshape(gy, levels, columns, LANES).transpose(1, 0, 2, 3)
    return out, warmed + returned.reshape(thermal_anomaly.shape)


def solution(mesh):
    return jax.shard_map(
        per_device,
        mesh=mesh,
        in_specs=(
            P(None, ("gx", "gy"), None, None),
            P(None, "gx", "gy"),
            P(None, "gx", "gy"),
            P(None, "gx", "gy"),
            P(None, "gx", "gy"),
            P("gx", "gy"),
            P(None, "gx", "gy"),
            P(("gx", "gy"), None),
            P(("gx", "gy"), None),
            P(),
            P(),
            P(),
            P(),
        ),
        out_specs=(P(None, ("gx", "gy"), None, None), P(None, "gx", "gy")),
        check_vma=False,
    )
```

```python
import functools

import jax
import jax.numpy as jnp
import numpy as np
from jax import lax
from jax.experimental import pallas as pl
from jax.experimental.pallas import tpu as pltpu
from jax.sharding import PartitionSpec as P


SUB = 3
NBIN = 8
NW = 4
SPREAD_FACTOR = 0.2

LANES = 128
MARGIN = 16
NEAR = 8
RIM = 2
CHUNKS = (1, 3, 2, 1, 1)

UV_ROWS = 24
MOIST_ROW = 48
DEPTH_ROW = 64
SUN_ROW = 80
EDGE_ROW = 88
FIELD_ROWS = 96
PAIRS = 20
SPAN = LANES + 2 * MARGIN
COEF_SPAN = LANES + 2 * NEAR


def spread_matrix():
    out = np.zeros((PAIRS, LANES, 2 * LANES), np.float32)
    for p in range(12):
        for part in range(3):
            out[p, 24 * part + p, :LANES] = 1.0
            out[p, 24 * part + 12 + p, LANES:] = 1.0
    for x in range(8):
        for part in range(3):
            out[12 + x, 72 + 8 * part + x, :LANES] = 1.0
        out[12 + x, 96 + x, LANES:] = 1.0
    return out


def hold(*arrays):
    return [pltpu.with_memory_space_constraint(x, pltpu.HBM) for x in arrays]


def three_parts(x):
    high = x.astype(jnp.bfloat16).astype(jnp.float32)
    rest = x - high
    middle = rest.astype(jnp.bfloat16).astype(jnp.float32)
    return [high, middle, rest - middle]


def chunk_rows(k):
    start = sum(CHUNKS[:k]) * LANES
    stop = start + CHUNKS[k] * LANES
    low = start - MARGIN if k == 0 else start + MARGIN
    return low, stop + (0 if k == len(CHUNKS) - 1 else MARGIN)


def slice_pieces(low, top):
    cuts = [low] + [c for c in range(-LANES, top, LANES) if low < c < top] + [top]
    return list(zip(cuts[:-1], cuts[1:]))


def slice_copies(chunks, place, tracer, outs, sems):
    mine = place[0]
    odd = lax.rem(mine, 2)
    blocks = tracer.shape[2] // LANES
    columns = tracer.shape[1]
    copies = []
    for n, k in enumerate(chunks):
        low, top = chunk_rows(k)
        for swap in range(2):
            upward = odd if swap else 1 - odd
            target = lax.rem(mine + 2 * upward - 1 + blocks, blocks)
            first = upward * (columns - SUB)
            for a, b in slice_pieces(low, top):
                block = lax.rem(target + 1 + (a // LANES) + blocks, blocks)
                row = pl.multiple_of(block * LANES + a % LANES, MARGIN)
                copies.append(
                    pltpu.make_async_copy(
                        tracer.at[:, pl.ds(first, SUB), pl.ds(row, b - a), :],
                        outs[2 * n + swap].at[:, :, a - low : b - low, :],
                        sems.at[len(copies)],
                    )
                )
    return copies


def copy_count(chunks):
    return sum(2 * len(slice_pieces(*chunk_rows(k))) for k in chunks)


def first_slice_kernel(place, tracer, u, v, warmth, out_0, out_1, rim_0, rim_1, sems):
    copies = slice_copies((0,), place, tracer, (out_0, out_1), sems)
    for copy in copies:
        copy.start()
    span = u.shape[1]
    odd = place[2] == 1

    def put(at, low, high):
        n = low.shape[0]
        rim_0[at : at + n, :] = jnp.where(odd, low, high)
        rim_1[at : at + n, :] = jnp.where(odd, high, low)

    for f in range(4):
        source = (u, v)[f // 2]
        put(RIM * f, source[f % 2, 0:RIM, :], source[f % 2, span - RIM : span, :])
    for level in range(2):
        put(4 * RIM + level, warmth[level, 0:1, :], warmth[level, span - 1 : span, :])
    at = 4 * RIM + 2
    for rim in (rim_0, rim_1):
        rim[at:, :] = jnp.zeros((rim.shape[0] - at, LANES), jnp.float32)
    for copy in copies:
        copy.wait()


def later_slice_kernel(place, tracer, *refs):
    later = tuple(range(1, len(CHUNKS)))
    n = 2 * len(later)
    outs, stages, sems, out_sems = refs[:n], refs[n : 2 * n], refs[2 * n], refs[2 * n + 1]
    copies = slice_copies(later, place, tracer, stages, sems)
    for copy in copies:
        copy.start()
    for copy in copies:
        copy.wait()
    copies = [pltpu.make_async_copy(stages[i], outs[i], out_sems.at[i]) for i in range(n)]
    for copy in copies:
        copy.start()
    for copy in copies:
        copy.wait()


def rims_of(place, rim_0, rim_1):
    odd = place[2] == 1
    return jnp.where(odd, rim_0[...], rim_1[...]), jnp.where(odd, rim_1[...], rim_0[...])


def pack_kernel(place, u, v, moisture, depth, sun, warmth, rim_0, rim_1, out, ext):
    mine = place[0]
    low, high = rims_of(place, rim_0, rim_1)
    parts = u.shape[1] // 8
    for f in range(4):
        source = (u, v)[f // 2]
        ext[f, 8 : 8 + u.shape[1], :] = source[f % 2]
        ext[f, 8 - RIM : 8, :] = low[RIM * f : RIM * (f + 1), :]
        ext[f, 8 + u.shape[1] : 8 + u.shape[1] + RIM, :] = high[RIM * f : RIM * (f + 1), :]
    turned = warmth[...].reshape(2 * u.shape[1], LANES).T
    last = turned[LANES - 1 :, :]
    initial = turned[:1, :]
    wide = 8 + 2 * RIM
    for d in range(parts):
        for level in range(2):
            base = UV_ROWS * level
            out[d, base : base + wide, :] = ext[level, 8 * d + 8 - RIM : 8 * d + 16 + RIM, :]
            out[d, base + wide : base + 2 * wide, :] = ext[
                2 + level, 8 * d + 8 - RIM : 8 * d + 16 + RIM, :
            ]
            out[d, MOIST_ROW + 8 * level : MOIST_ROW + 8 * level + 8, :] = moisture[
                level, 8 * d : 8 * d + 8, :
            ]
            out[d, DEPTH_ROW + 8 * level : DEPTH_ROW + 8 * level + 8, :] = depth[
                level, 8 * d : 8 * d + 8, :
            ]
        out[d, SUN_ROW : SUN_ROW + 8, :] = sun[8 * d : 8 * d + 8, :]
        row = jnp.where(mine + 1 == d, last, jnp.where(mine - 1 == d, initial, 0.0))
        out[d, EDGE_ROW : EDGE_ROW + 8, :] = jnp.broadcast_to(row, (8, LANES))


def turn_kernel(fields, kind, bins, turned, classes):
    for block in range(fields.shape[0]):
        lanes = slice(block * LANES, (block + 1) * LANES)
        classes[block] = bins[:, lanes]
        for level in range(2):
            parts = three_parts(fields[block, UV_ROWS * level : UV_ROWS * (level + 1), :])
            if level == 0:
                parts += three_parts(fields[block, DEPTH_ROW : DEPTH_ROW + 8, :])
                parts.append(kind[:, lanes].astype(jnp.float32))
                parts.append(jnp.zeros((24, LANES), jnp.float32))
            else:
                parts.append(jnp.zeros((56, LANES), jnp.float32))
            turned[level, block] = jnp.concatenate(parts, axis=0).T.astype(jnp.bfloat16)


def warm_kernel(place, warmth, rim_0, rim_1, fields, out, ext):
    mine = place[0]
    low, high = rims_of(place, rim_0, rim_1)
    tiles = fields.shape[0]
    span = warmth.shape[1]
    lane = lax.broadcasted_iota(jnp.int32, (span, LANES), 1)
    left = fields[jnp.maximum(mine - 1, 0), EDGE_ROW : EDGE_ROW + 1, :]
    right = fields[jnp.minimum(mine + 1, tiles - 1), EDGE_ROW : EDGE_ROW + 1, :]
    at = 4 * RIM
    for level in range(2):
        here = warmth[level]
        ext[8 : 8 + span, :] = here
        ext[7:8, :] = low[at + level : at + level + 1, :]
        ext[8 + span : 9 + span, :] = high[at + level : at + level + 1, :]
        left_rows = jnp.broadcast_to(left[:, level * span : (level + 1) * span], (LANES, span)).T
        right_rows = jnp.broadcast_to(right[:, level * span : (level + 1) * span], (LANES, span)).T
        west = jnp.where(lane == 0, left_rows, pltpu.roll(here, 1, 1))
        east = jnp.where(lane == LANES - 1, right_rows, pltpu.roll(here, LANES - 1, 1))
        laplace = ext[9 : 9 + span, :] + ext[7 : 7 + span, :] + east + west - 4.0 * here
        out[level] = here + SPREAD_FACTOR * laplace


def block_lhs(turned, level, block, blocks):
    low = turned[level, jnp.maximum(block - 1, 0), LANES - MARGIN :, :].astype(jnp.float32)
    high = turned[level, jnp.minimum(block + 1, blocks - 1), :MARGIN, :].astype(jnp.float32)
    low = low * jnp.where(block != 0, 1.0, 0.0)
    high = high * jnp.where(block != blocks - 1, 1.0, 0.0)
    ends = [low.astype(jnp.bfloat16), high.astype(jnp.bfloat16)]
    return jnp.concatenate([ends[0], turned[level, block], ends[1]], axis=0)


def coefficient_kernel(turned, spread, speeds, coef, share, stage, hot, kept, sems, share_sem):
    blocks = coef.shape[0]
    lane = lax.broadcasted_iota(jnp.int32, (1, LANES), 1)
    category = jnp.where(lane < 72, lane % 24, -1).astype(jnp.float32)
    columns = share.shape[1]

    def copies(block, level):
        these = [pltpu.make_async_copy(stage.at[level], coef.at[block, level], sems.at[level])]
        if level == 0:
            these.append(pltpu.make_async_copy(kept, share.at[block], share_sem.at[0]))
        return these

    def one_block(block, carry):
        for level in (1, 0):

            @pl.when(block > 0)
            def _():
                for copy in copies(block - 1, level):
                    copy.wait()

            lhs = block_lhs(turned, level, block, blocks)
            for c in range(stage.shape[1] // 2):
                both = jnp.dot(lhs, spread[c], preferred_element_type=jnp.float32)
                stage[level, 2 * c] = both[NEAR : NEAR + COEF_SPAN, :LANES]
                stage[level, 2 * c + 1] = both[NEAR : NEAR + COEF_SPAN, LANES:]
            if level == 0:
                middle = lhs[MARGIN : MARGIN + LANES]
                for x in range(columns):
                    pair = jnp.dot(middle, spread[12 + x], preferred_element_type=jnp.float32)
                    kept[x] = pair[:, :LANES]
                    hot[x] = jnp.where(pair[:, LANES:] == category, 1.0, 0.0).astype(jnp.bfloat16)
                for x in range(columns):
                    speed = jnp.dot(hot[x], speeds[...], preferred_element_type=jnp.float32)
                    kept[x] = kept[x] / (kept[x] + speed)
            for copy in copies(block, level):
                copy.start()
        return carry

    lax.fori_loop(0, blocks, one_block, 0)
    for level in (1, 0):
        for copy in copies(blocks - 1, level):
            copy.wait()


def row_blocks(first, count, size):
    return [(r, min(size, first + count - r)) for r in range(first, first + count, size)]


def chunk_kernel(k, *refs):
    first, final = k == 0, k == len(CHUNKS) - 1
    count = CHUNKS[k]
    refs = list(refs)
    place, sunlight, table, fields, classes, tracer, all_coef, all_share = refs[:8]
    del refs[:8]
    halos = refs[:2]
    del refs[:2]
    before = (None, None)
    if not first:
        before = refs[:2]
        del refs[:2]
        around = (None, None)
        if final:
            around = refs[:2]
            del refs[:2]
            del refs[:1]
        else:
            del refs[:2]
    out, heat = refs[:2]
    window, even, odd, coef, kept, result, thick, warm = refs[2:10]
    in_sems, coef_sems, out_sems, heat_sems = refs[10:]

    columns = 8
    wide = columns + 2 * SUB
    mine, z = place[0], place[1]
    parity = lax.rem(mine, 2)
    blocks = out.shape[2] // LANES
    grid_rows = out.shape[2]
    top = MARGIN + LANES

    sublane = lax.broadcasted_iota(jnp.int32, (8, LANES), 0)
    weights = jnp.zeros((8, LANES), jnp.float32)
    for w in range(NW):
        weights = jnp.where(sublane == NW + w, sunlight[w], weights)

    def wide_of(x):
        return x.astype(jnp.float32)

    def loads(j, slot, level):
        block = lax.rem(mine + 1 + sum(CHUNKS[:k]) + j, blocks)
        row = pl.multiple_of(block * LANES, LANES)
        low = pl.multiple_of(jnp.maximum(row - MARGIN, 0), MARGIN)
        high = pl.multiple_of(jnp.minimum(row + LANES, grid_rows - MARGIN), MARGIN)
        return [
            pltpu.make_async_copy(
                tracer.at[level, :, pl.ds(at, n), :],
                window.at[slot, level, :, to : to + n, :],
                in_sems.at[slot, level, i],
            )
            for i, (at, to, n) in enumerate(
                ((low, 0, MARGIN), (row, MARGIN, LANES), (high, MARGIN + LANES, MARGIN))
            )
        ]

    def load_block(j, slot):
        for level in (1, 0):
            for copy in loads(j, slot, level):
                copy.start()

    def coef_loads(j, level):
        block = lax.rem(mine + 1 + sum(CHUNKS[:k]) + j, blocks)
        these = [
            pltpu.make_async_copy(all_coef.at[block, level], coef.at[level], coef_sems.at[level])
        ]
        if level == 0:
            these.append(pltpu.make_async_copy(all_share.at[block], kept, coef_sems.at[2]))
        return these

    def copies(j, slot, which=None):
        block = lax.rem(mine + 1 + sum(CHUNKS[:k]) + j, blocks)
        row = pl.multiple_of(block * LANES, LANES)
        these = []
        for level in (0, 1) if which is None else (which,):
            if level < 2:
                source, target = result.at[slot, level], out.at[level, :, pl.ds(row, LANES), :]
                these.append(pltpu.make_async_copy(source, target, out_sems.at[slot, level]))
        if which == 2 or (which is None and not final):
            these.append(pltpu.make_async_copy(warm.at[slot], heat.at[block], heat_sems.at[slot]))
        return these

    def field_row(block, at):
        return fields[block, at : at + 1, :]

    def step(level, source, c, i, r0, n):
        here = source[c, r0 : r0 + n, :]
        u = coef[level, 2 * i, r0 - NEAR : r0 - NEAR + n, :]
        v = coef[level, 2 * i + 1, r0 - NEAR : r0 - NEAR + n, :]
        across = jnp.where(u > 0.0, source[c - 1, r0 : r0 + n, :], source[c + 1, r0 : r0 + n, :])
        along = jnp.where(
            v > 0.0, source[c, pl.ds(z + (r0 - 1), n), :], source[c, pl.ds(z + (r0 + 1), n), :]
        )
        return here - jnp.abs(u) * (here - across) - jnp.abs(v) * (here - along)

    def one_block(j, carry):
        slot = lax.rem(j, 2)
        block = lax.rem(mine + 1 + sum(CHUNKS[:k]) + j, blocks)
        has_low = jnp.where(block != 0, 1.0, 0.0)
        has_high = jnp.where(block != blocks - 1, 1.0, 0.0)

        if count > 1:

            @pl.when(j + 1 < count)
            def _():
                load_block(j + 1, 1 - slot)

        if count > 2:

            @pl.when(j >= 2)
            def _():
                for copy in copies(j - 2, slot):
                    copy.wait()

        for level in (1, 0):
            def widen(at, low, head, tail, high):
                even[at, NEAR:MARGIN, :] = wide_of(low)[NEAR:, :] * has_low
                even[at, MARGIN : 2 * MARGIN, :] = wide_of(head)
                even[at, 2 * MARGIN : top, :] = wide_of(tail)
                even[at, top : top + NEAR, :] = wide_of(high)[:NEAR, :] * has_high

            for copy in loads(j, slot, level):
                copy.wait()

            def widen_column(x, carry):
                parts = [
                    window[slot, level, x, r : r + n, :]
                    for r, n in (
                        (0, MARGIN),
                        (MARGIN, MARGIN),
                        (2 * MARGIN, LANES - MARGIN),
                        (top, MARGIN),
                    )
                ]
                widen(SUB + x, *parts)
                return carry

            lax.fori_loop(0, columns, widen_column, 0)

            def rims(at_start):
                for swap, (rim, prior) in enumerate(zip(halos, before)):
                    for c in range(SUB):
                        at = c + (parity if swap else 1 - parity) * (SUB + columns)
                        if at_start:
                            end = prior.shape[2]
                            low = prior[level, c, end - 2 * MARGIN : end - MARGIN, :]
                            head = prior[level, c, end - MARGIN : end, :]
                            tail = rim[level, c, 0 : LANES - MARGIN, :]
                            if final:
                                high = around[swap][level, c, MARGIN : 2 * MARGIN, :]
                            else:
                                high = rim[level, c, LANES - MARGIN : LANES, :]
                        else:
                            base = j * LANES + (0 if first else -2 * MARGIN)
                            low, head, tail, high = (
                                rim[level, c, pl.ds(pl.multiple_of(base + a, MARGIN), n), :]
                                for a, n in (
                                    (0, MARGIN),
                                    (MARGIN, MARGIN),
                                    (2 * MARGIN, LANES - MARGIN),
                                    (top, MARGIN),
                                )
                            )
                        widen(at, low, head, tail, high)

            if first:
                rims(False)
            elif count == 1:
                rims(True)
            else:
                pl.when(j == 0)(functools.partial(rims, True))
                pl.when(j != 0)(functools.partial(rims, False))

            def substep_one(c, carry):
                for r0, n in row_blocks(NEAR, LANES + 2 * NEAR, 72):
                    odd[c, r0 : r0 + n, :] = step(level, even, c, c - 1, r0, n)
                return carry

            def substep_two(c, carry):
                for r0, n in row_blocks(NEAR, LANES + 2 * NEAR, 72):
                    even[c, r0 : r0 + n, :] = step(level, odd, c, c - 1, r0, n)
                return carry

            for copy in coef_loads(j, level):
                copy.wait()
            lax.fori_loop(1, wide - 1, substep_one, 0)
            lax.fori_loop(2, wide - 2, substep_two, 0)

            def substep_three(x, carry):
                c = x + SUB
                for r0, n in row_blocks(MARGIN, LANES, 64):
                    now = step(level, even, c, c - 1, r0, n)
                    if level == 0:
                        now = now * kept[x, r0 - MARGIN : r0 - MARGIN + n, :]
                    result[slot, level, x, r0 - MARGIN : r0 - MARGIN + n, :] = now
                return carry

            lax.fori_loop(0, columns, substep_three, 0)
            copies(j, slot, level)[0].start()
            if count > 1:

                @pl.when(j + 1 < count)
                def _():
                    for copy in coef_loads(j + 1, level):
                        copy.start()

            for x in range(columns):
                rounded = result[slot, level, x].astype(jnp.bfloat16)
                projected = lax.dot_general(
                    table[...], rounded, (((1,), (1,)), ((), ())), preferred_element_type=jnp.float32
                )
                which = classes[block, x : x + 1, :]
                dry = jnp.zeros((8, LANES), jnp.float32)
                wet = jnp.zeros((8, LANES), jnp.float32)
                for b in range(NBIN):
                    dry = jnp.where(which == b, projected[8 * b : 8 * b + 8], dry)
                    wet = jnp.where(which == b, projected[64 + 8 * b : 72 + 8 * b], wet)
                at = 8 * level + x
                moist = field_row(block, MOIST_ROW + at)
                thickness = field_row(block, DEPTH_ROW + at)
                sun = field_row(block, SUN_ROW + x)
                growth = moist / (1.0 - moist)
                optical = (dry + growth * wet) * thickness
                if level == 1:
                    thick[x] = optical
                    lit = weights * optical
                else:
                    overhead = pltpu.roll(thick[x], NW, 0)
                    lit = weights * optical * jnp.exp(-overhead / sun)
                lit = sun * jnp.sum(lit, axis=0, keepdims=True)
                if final:
                    heat[at : at + 1, :] = lit
                else:
                    warm[slot, at : at + 1, :] = lit
        if not final:
            copies(j, slot, 2)[0].start()
        return carry

    load_block(0, 0)
    for level in (1, 0):
        for copy in coef_loads(0, level):
            copy.start()
    if count == 1:
        one_block(0, 0)
    else:
        lax.fori_loop(0, count, one_block, 0)
    for j in range(max(count - 2, 0), count):
        for copy in copies(j, j % 2):
            copy.wait()
    if first:
        copy = pltpu.make_async_copy(warm.at[0], heat.at[mine], heat_sems.at[0])
        copy.start()
        copy.wait()


def chunk_call(k, operands, out, heat, shape, gy):
    first, final = k == 0, k == len(CHUNKS) - 1
    levels, columns, _, _ = shape
    vmem = pl.BlockSpec(memory_space=pltpu.VMEM)
    smem = pl.BlockSpec(memory_space=pltpu.SMEM)
    hbm = pl.BlockSpec(memory_space=pltpu.HBM)
    operands = list(operands)
    specs = [smem, smem] + [vmem] * 3 + [hbm] * 3 + [vmem] * (len(operands) - 8)
    heat_block = (levels * columns, LANES)
    out_shapes = [jax.ShapeDtypeStruct(shape, jnp.float32)]
    out_specs = [hbm]
    aliases = {}
    if not first:
        aliases[len(operands)] = 0
        operands.append(out)
        specs.append(hbm)
    if final:
        out_shapes.append(jax.ShapeDtypeStruct(heat_block, jnp.float32))
        out_specs.append(vmem)
    else:
        if not first:
            aliases[len(operands)] = 1
            operands.append(heat)
            specs.append(hbm)
        out_shapes.append(jax.ShapeDtypeStruct((gy,) + heat_block, jnp.float32))
        out_specs.append(hbm)
    work = CHUNKS[k] * LANES * columns * levels * LANES
    return pl.pallas_call(
        functools.partial(chunk_kernel, k),
        out_shape=tuple(out_shapes),
        in_specs=specs,
        out_specs=tuple(out_specs),
        scratch_shapes=[
            pltpu.VMEM((2, levels, columns, SPAN, LANES), jnp.bfloat16),
            pltpu.VMEM((columns + 2 * SUB, SPAN, LANES), jnp.float32),
            pltpu.VMEM((columns + 2 * SUB, SPAN, LANES), jnp.float32),
            pltpu.VMEM((levels, 24, COEF_SPAN, LANES), jnp.float32),
            pltpu.VMEM((columns, LANES, LANES), jnp.float32),
            pltpu.VMEM((2, levels, columns, LANES, LANES), jnp.float32),
            pltpu.VMEM((columns, 8, LANES), jnp.float32),
            pltpu.VMEM((2, levels * columns, LANES), jnp.float32),
            pltpu.SemaphoreType.DMA((2, levels, 3)),
            pltpu.SemaphoreType.DMA((3,)),
            pltpu.SemaphoreType.DMA((2, levels)),
            pltpu.SemaphoreType.DMA((2,)),
        ],
        input_output_aliases=aliases,
        compiler_params=pltpu.CompilerParams(vmem_limit_bytes=12 * 1024 * 1024),
        cost_estimate=pl.CostEstimate(flops=60 * work, transcendentals=0, bytes_accessed=8 * work),
    )(*operands)


def per_device(
    tracer_amounts,
    zonal_transit_ratio,
    meridional_transit_ratio,
    moisture_ratio,
    stratum_depths,
    sun_elevation_factor,
    thermal_anomaly,
    particle_class_map,
    ground_cover_kind,
    arid_extinction_table,
    swelling_factors,
    settling_velocities,
    arriving_irradiance,
):
    f32, bf16 = jnp.float32, jnp.bfloat16
    levels, columns, _, species = tracer_amounts.shape
    tile = thermal_anomaly.shape[1]
    gx, gy = lax.axis_size("gx"), lax.axis_size("gy")
    strips = ("gx", "gy")

    def swaps(n):
        pairs = [[(i, i + 1) for i in range(start, n - 1, 2)] for start in (0, 1)]
        return [p + [(j, i) for i, j in p] for p in pairs]

    vmem = pl.BlockSpec(memory_space=pltpu.VMEM)
    smem = pl.BlockSpec(memory_space=pltpu.SMEM)
    hbm = pl.BlockSpec(memory_space=pltpu.HBM)

    mine = lax.axis_index("gy").astype(jnp.int32)
    gx_odd = lax.rem(lax.axis_index("gx").astype(jnp.int32), 2)
    place = jnp.stack([mine, jnp.zeros((), jnp.int32), gx_odd])

    def halo_shape(k):
        low, high = chunk_rows(k)
        return jax.ShapeDtypeStruct((levels, SUB, high - low, species), bf16)

    rim_shape = jax.ShapeDtypeStruct((2 * 8, LANES), f32)
    *slices, rim_0, rim_1 = pl.pallas_call(
        first_slice_kernel,
        out_shape=(halo_shape(0), halo_shape(0), rim_shape, rim_shape),
        in_specs=[smem, hbm] + [vmem] * 3,
        out_specs=(vmem,) * 4,
        scratch_shapes=[pltpu.SemaphoreType.DMA((copy_count((0,)),))],
        compiler_params=pltpu.CompilerParams(vmem_limit_bytes=4 * 1024 * 1024),
        name="slice_first",
    )(
        place,
        *hold(tracer_amounts, zonal_transit_ratio, meridional_transit_ratio, thermal_anomaly),
    )
    later = tuple(range(1, len(CHUNKS)))
    later_shapes = [halo_shape(k) for k in later for _ in range(2)]
    slices += hold(
        *pl.pallas_call(
            later_slice_kernel,
            out_shape=tuple(pltpu.HBM(x.shape, x.dtype) for x in later_shapes),
            in_specs=[smem, hbm],
            out_specs=(hbm,) * len(later_shapes),
            scratch_shapes=[pltpu.VMEM(x.shape, x.dtype) for x in later_shapes]
            + [
                pltpu.SemaphoreType.DMA((copy_count(later),)),
                pltpu.SemaphoreType.DMA((len(later_shapes),)),
            ],
            compiler_params=pltpu.CompilerParams(vmem_limit_bytes=8 * 1024 * 1024),
            name="slice_later",
        )(place, *hold(tracer_amounts))
    )

    rims = [lax.ppermute(r, "gx", p) for r, p in zip((rim_0, rim_1), swaps(gx))]
    halos = []
    for k in range(len(CHUNKS)):
        pair = slices[2 * k : 2 * k + 2]
        halos.append([lax.ppermute(h, strips, p) for h, p in zip(pair, swaps(gx * gy))])

    packed = pl.pallas_call(
        pack_kernel,
        out_shape=jax.ShapeDtypeStruct((gy, FIELD_ROWS, LANES), f32),
        in_specs=[smem] + [vmem] * 8,
        out_specs=vmem,
        scratch_shapes=[pltpu.VMEM((4, tile + 16, LANES), f32)],
        compiler_params=pltpu.CompilerParams(vmem_limit_bytes=4 * 1024 * 1024),
        name="pack",
    )(
        place,
        *hold(
            zonal_transit_ratio,
            meridional_transit_ratio,
            moisture_ratio,
            stratum_depths,
            sun_elevation_factor,
            thermal_anomaly,
        ),
        *rims,
    )
    fields = lax.all_to_all(packed, "gy", split_axis=0, concat_axis=0, tiled=True)

    turned, classes = pl.pallas_call(
        turn_kernel,
        out_shape=(
            jax.ShapeDtypeStruct((levels, gy, LANES, LANES), bf16),
            jax.ShapeDtypeStruct((gy, columns, LANES), jnp.int32),
        ),
        in_specs=[vmem] * 3,
        out_specs=(vmem, vmem),
        compiler_params=pltpu.CompilerParams(vmem_limit_bytes=4 * 1024 * 1024),
        name="turn",
    )(fields, *hold(ground_cover_kind, particle_class_map))

    warmed = pl.pallas_call(
        warm_kernel,
        out_shape=jax.ShapeDtypeStruct(thermal_anomaly.shape, f32),
        in_specs=[smem] + [vmem] * 4,
        out_specs=vmem,
        scratch_shapes=[pltpu.VMEM((tile + 16, LANES), f32)],
        compiler_params=pltpu.CompilerParams(vmem_limit_bytes=4 * 1024 * 1024),
        name="warm",
    )(place, *hold(thermal_anomaly), *rims, fields)

    spread = jnp.asarray(spread_matrix(), bf16)
    table = jnp.concatenate([arid_extinction_table, swelling_factors], axis=1).T
    parts, rest = [], settling_velocities
    for _ in range(3):
        part = lax.reduce_precision(rest, 8, 7)
        parts.append(part.astype(bf16))
        rest = rest - part
    parts.append(jnp.zeros((LANES - 3 * settling_velocities.shape[0], species), bf16))
    speeds = jnp.concatenate(parts, axis=0)

    coef_shape = (24, LANES + 2 * NEAR, LANES)
    coefficients = pl.pallas_call(
        coefficient_kernel,
        out_shape=(
            pltpu.HBM((gy, levels) + coef_shape, f32),
            pltpu.HBM((gy, columns, LANES, LANES), f32),
        ),
        in_specs=[vmem] * 3,
        out_specs=(hbm, hbm),
        scratch_shapes=[
            pltpu.VMEM((levels,) + coef_shape, f32),
            pltpu.VMEM((columns, LANES, LANES), bf16),
            pltpu.VMEM((columns, LANES, LANES), f32),
            pltpu.SemaphoreType.DMA((levels,)),
            pltpu.SemaphoreType.DMA((1,)),
        ],
        compiler_params=pltpu.CompilerParams(vmem_limit_bytes=12 * 1024 * 1024),
        name="coefficients",
    )(turned, spread, speeds)

    def run_chunk(k, out, heat):
        operands = [table, fields, classes]
        final = k == len(CHUNKS) - 1
        for n in [k] + [k - 1] * (k > 0) + [0] * final:
            operands += halos[n]
        if final:
            operands = hold(*operands)
        held = hold(tracer_amounts, *coefficients)
        operands = [place, arriving_irradiance] + operands[:3] + held + operands[3:]
        return chunk_call(k, operands, out, heat, tracer_amounts.shape, gy)

    out = heat = None
    for k in range(len(CHUNKS) - 1):
        out, heat = run_chunk(k, out, heat)
    returned = lax.all_to_all(heat, "gy", split_axis=0, concat_axis=0, tiled=True)
    out, own = run_chunk(len(CHUNKS) - 1, out, None)

    is_own = lax.broadcasted_iota(jnp.int32, (gy, 1, 1), 0) == mine
    returned = jnp.where(is_own, own[None], returned)
    returned = returned.reshape(gy, levels, columns, LANES).transpose(1, 0, 2, 3)
    return out, warmed + returned.reshape(thermal_anomaly.shape)


def solution(mesh):
    return jax.shard_map(
        per_device,
        mesh=mesh,
        in_specs=(
            P(None, ("gx", "gy"), None, None),
            P(None, "gx", "gy"),
            P(None, "gx", "gy"),
            P(None, "gx", "gy"),
            P(None, "gx", "gy"),
            P("gx", "gy"),
            P(None, "gx", "gy"),
            P(("gx", "gy"), None),
            P(("gx", "gy"), None),
            P(),
            P(),
            P(),
            P(),
        ),
        out_specs=(P(None, ("gx", "gy"), None, None), P(None, "gx", "gy")),
        check_vma=False,
    )
```

```python
import functools

import jax
import jax.numpy as jnp
import numpy as np
from jax import lax
from jax.experimental import pallas as pl
from jax.experimental.pallas import tpu as pltpu
from jax.sharding import PartitionSpec as P


SUB = 3
NBIN = 8
NW = 4
SPREAD_FACTOR = 0.2

LANES = 128
MARGIN = 16
NEAR = 8
RIM = 2
CHUNKS = (1, 4, 2, 1)

UV_ROWS = 24
MOIST_ROW = 48
DEPTH_ROW = 64
SUN_ROW = 80
EDGE_ROW = 88
FIELD_ROWS = 96
PAIRS = 20
SPAN = LANES + 2 * MARGIN
COEF_SPAN = LANES + 2 * NEAR


def spread_matrix():
    out = np.zeros((PAIRS, LANES, 2 * LANES), np.float32)
    for p in range(12):
        for part in range(3):
            out[p, 24 * part + p, :LANES] = 1.0
            out[p, 24 * part + 12 + p, LANES:] = 1.0
    for x in range(8):
        for part in range(3):
            out[12 + x, 72 + 8 * part + x, :LANES] = 1.0
        out[12 + x, 96 + x, LANES:] = 1.0
    return out


def hold(*arrays):
    return [pltpu.with_memory_space_constraint(x, pltpu.HBM) for x in arrays]


def three_parts(x):
    high = x.astype(jnp.bfloat16).astype(jnp.float32)
    rest = x - high
    middle = rest.astype(jnp.bfloat16).astype(jnp.float32)
    return [high, middle, rest - middle]


def chunk_rows(k):
    start = sum(CHUNKS[:k]) * LANES
    stop = start + CHUNKS[k] * LANES
    low = start - MARGIN if k == 0 else start + MARGIN
    return low, stop + (0 if k == len(CHUNKS) - 1 else MARGIN)


def slice_pieces(low, top):
    cuts = [low] + [c for c in range(-LANES, top, LANES) if low < c < top] + [top]
    return list(zip(cuts[:-1], cuts[1:]))


def slice_copies(chunks, place, tracer, outs, sems):
    mine = place[0]
    odd = lax.rem(mine, 2)
    blocks = tracer.shape[2] // LANES
    columns = tracer.shape[1]
    copies = []
    for n, k in enumerate(chunks):
        low, top = chunk_rows(k)
        for swap in range(2):
            upward = odd if swap else 1 - odd
            target = lax.rem(mine + 2 * upward - 1 + blocks, blocks)
            first = upward * (columns - SUB)
            for a, b in slice_pieces(low, top):
                block = lax.rem(target + 1 + (a // LANES) + blocks, blocks)
                row = pl.multiple_of(block * LANES + a % LANES, MARGIN)
                copies.append(
                    pltpu.make_async_copy(
                        tracer.at[:, pl.ds(first, SUB), pl.ds(row, b - a), :],
                        outs[2 * n + swap].at[:, :, a - low : b - low, :],
                        sems.at[len(copies)],
                    )
                )
    return copies


def copy_count(chunks):
    return sum(2 * len(slice_pieces(*chunk_rows(k))) for k in chunks)


def first_slice_kernel(place, tracer, u, v, warmth, out_0, out_1, rim_0, rim_1, sems):
    copies = slice_copies((0,), place, tracer, (out_0, out_1), sems)
    for copy in copies:
        copy.start()
    span = u.shape[1]
    odd = place[2] == 1

    def put(at, low, high):
        n = low.shape[0]
        rim_0[at : at + n, :] = jnp.where(odd, low, high)
        rim_1[at : at + n, :] = jnp.where(odd, high, low)

    for f in range(4):
        source = (u, v)[f // 2]
        put(RIM * f, source[f % 2, 0:RIM, :], source[f % 2, span - RIM : span, :])
    for level in range(2):
        put(4 * RIM + level, warmth[level, 0:1, :], warmth[level, span - 1 : span, :])
    at = 4 * RIM + 2
    for rim in (rim_0, rim_1):
        rim[at:, :] = jnp.zeros((rim.shape[0] - at, LANES), jnp.float32)
    for copy in copies:
        copy.wait()


def later_slice_kernel(place, tracer, *refs):
    later = tuple(range(1, len(CHUNKS)))
    n = 2 * len(later)
    outs, stages, sems, out_sems = refs[:n], refs[n : 2 * n], refs[2 * n], refs[2 * n + 1]
    copies = slice_copies(later, place, tracer, stages, sems)
    for copy in copies:
        copy.start()
    for copy in copies:
        copy.wait()
    copies = [pltpu.make_async_copy(stages[i], outs[i], out_sems.at[i]) for i in range(n)]
    for copy in copies:
        copy.start()
    for copy in copies:
        copy.wait()


def rims_of(place, rim_0, rim_1):
    odd = place[2] == 1
    return jnp.where(odd, rim_0[...], rim_1[...]), jnp.where(odd, rim_1[...], rim_0[...])


def pack_kernel(place, u, v, moisture, depth, sun, warmth, rim_0, rim_1, out, ext):
    mine = place[0]
    low, high = rims_of(place, rim_0, rim_1)
    parts = u.shape[1] // 8
    for f in range(4):
        source = (u, v)[f // 2]
        ext[f, 8 : 8 + u.shape[1], :] = source[f % 2]
        ext[f, 8 - RIM : 8, :] = low[RIM * f : RIM * (f + 1), :]
        ext[f, 8 + u.shape[1] : 8 + u.shape[1] + RIM, :] = high[RIM * f : RIM * (f + 1), :]
    turned = warmth[...].reshape(2 * u.shape[1], LANES).T
    last = turned[LANES - 1 :, :]
    initial = turned[:1, :]
    wide = 8 + 2 * RIM
    for d in range(parts):
        for level in range(2):
            base = UV_ROWS * level
            out[d, base : base + wide, :] = ext[level, 8 * d + 8 - RIM : 8 * d + 16 + RIM, :]
            out[d, base + wide : base + 2 * wide, :] = ext[
                2 + level, 8 * d + 8 - RIM : 8 * d + 16 + RIM, :
            ]
            out[d, MOIST_ROW + 8 * level : MOIST_ROW + 8 * level + 8, :] = moisture[
                level, 8 * d : 8 * d + 8, :
            ]
            out[d, DEPTH_ROW + 8 * level : DEPTH_ROW + 8 * level + 8, :] = depth[
                level, 8 * d : 8 * d + 8, :
            ]
        out[d, SUN_ROW : SUN_ROW + 8, :] = sun[8 * d : 8 * d + 8, :]
        row = jnp.where(mine + 1 == d, last, jnp.where(mine - 1 == d, initial, 0.0))
        out[d, EDGE_ROW : EDGE_ROW + 8, :] = jnp.broadcast_to(row, (8, LANES))


def turn_kernel(fields, kind, bins, turned, classes):
    for block in range(fields.shape[0]):
        lanes = slice(block * LANES, (block + 1) * LANES)
        classes[block] = bins[:, lanes]
        for level in range(2):
            parts = three_parts(fields[block, UV_ROWS * level : UV_ROWS * (level + 1), :])
            if level == 0:
                parts += three_parts(fields[block, DEPTH_ROW : DEPTH_ROW + 8, :])
                parts.append(kind[:, lanes].astype(jnp.float32))
                parts.append(jnp.zeros((24, LANES), jnp.float32))
            else:
                parts.append(jnp.zeros((56, LANES), jnp.float32))
            turned[level, block] = jnp.concatenate(parts, axis=0).T.astype(jnp.bfloat16)


def warm_kernel(place, warmth, rim_0, rim_1, fields, out, ext):
    mine = place[0]
    low, high = rims_of(place, rim_0, rim_1)
    tiles = fields.shape[0]
    span = warmth.shape[1]
    lane = lax.broadcasted_iota(jnp.int32, (span, LANES), 1)
    left = fields[jnp.maximum(mine - 1, 0), EDGE_ROW : EDGE_ROW + 1, :]
    right = fields[jnp.minimum(mine + 1, tiles - 1), EDGE_ROW : EDGE_ROW + 1, :]
    at = 4 * RIM
    for level in range(2):
        here = warmth[level]
        ext[8 : 8 + span, :] = here
        ext[7:8, :] = low[at + level : at + level + 1, :]
        ext[8 + span : 9 + span, :] = high[at + level : at + level + 1, :]
        left_rows = jnp.broadcast_to(left[:, level * span : (level + 1) * span], (LANES, span)).T
        right_rows = jnp.broadcast_to(right[:, level * span : (level + 1) * span], (LANES, span)).T
        west = jnp.where(lane == 0, left_rows, pltpu.roll(here, 1, 1))
        east = jnp.where(lane == LANES - 1, right_rows, pltpu.roll(here, LANES - 1, 1))
        laplace = ext[9 : 9 + span, :] + ext[7 : 7 + span, :] + east + west - 4.0 * here
        out[level] = here + SPREAD_FACTOR * laplace


def block_lhs(turned, level, block, blocks):
    low = turned[level, jnp.maximum(block - 1, 0), LANES - MARGIN :, :].astype(jnp.float32)
    high = turned[level, jnp.minimum(block + 1, blocks - 1), :MARGIN, :].astype(jnp.float32)
    low = low * jnp.where(block != 0, 1.0, 0.0)
    high = high * jnp.where(block != blocks - 1, 1.0, 0.0)
    ends = [low.astype(jnp.bfloat16), high.astype(jnp.bfloat16)]
    return jnp.concatenate([ends[0], turned[level, block], ends[1]], axis=0)


def coefficient_kernel(turned, spread, speeds, coef, share, stage, hot, kept, sems, share_sem):
    blocks = coef.shape[0]
    lane = lax.broadcasted_iota(jnp.int32, (1, LANES), 1)
    category = jnp.where(lane < 72, lane % 24, -1).astype(jnp.float32)
    columns = share.shape[1]

    def copies(block, level):
        these = [pltpu.make_async_copy(stage.at[level], coef.at[block, level], sems.at[level])]
        if level == 0:
            these.append(pltpu.make_async_copy(kept, share.at[block], share_sem.at[0]))
        return these

    def one_block(block, carry):
        for level in (1, 0):

            @pl.when(block > 0)
            def _():
                for copy in copies(block - 1, level):
                    copy.wait()

            lhs = block_lhs(turned, level, block, blocks)
            for c in range(stage.shape[1] // 2):
                both = jnp.dot(lhs, spread[c], preferred_element_type=jnp.float32)
                stage[level, 2 * c] = both[NEAR : NEAR + COEF_SPAN, :LANES]
                stage[level, 2 * c + 1] = both[NEAR : NEAR + COEF_SPAN, LANES:]
            if level == 0:
                middle = lhs[MARGIN : MARGIN + LANES]
                for x in range(columns):
                    pair = jnp.dot(middle, spread[12 + x], preferred_element_type=jnp.float32)
                    kept[x] = pair[:, :LANES]
                    hot[x] = jnp.where(pair[:, LANES:] == category, 1.0, 0.0).astype(jnp.bfloat16)
                for x in range(columns):
                    speed = jnp.dot(hot[x], speeds[...], preferred_element_type=jnp.float32)
                    kept[x] = kept[x] / (kept[x] + speed)
            for copy in copies(block, level):
                copy.start()
        return carry

    lax.fori_loop(0, blocks, one_block, 0)
    for level in (1, 0):
        for copy in copies(blocks - 1, level):
            copy.wait()


def row_blocks(first, count, size):
    return [(r, min(size, first + count - r)) for r in range(first, first + count, size)]


def chunk_kernel(k, *refs):
    first, final = k == 0, k == len(CHUNKS) - 1
    count = CHUNKS[k]
    refs = list(refs)
    place, sunlight = refs[:2]
    sources, (tracer, all_coef, all_share) = refs[2:5], refs[5:8]
    del refs[:8]
    table, fields, classes = refs[-3:]
    del refs[-3:]
    sources += refs[:2]
    del refs[:2]
    halos = refs[-2:]
    del refs[-2:]
    targets = [table, fields, classes, *halos]
    before = (None, None)
    if not first:
        end = refs[0].shape[2]
        sources += [r.at[:, :, end - 2 * MARGIN : end, :] for r in refs[:2]]
        del refs[:2]
        before = refs[-2:]
        del refs[-2:]
        targets += before
        around = (None, None)
        if final:
            sources += [r.at[:, :, MARGIN : 2 * MARGIN, :] for r in refs[:2]]
            del refs[:2]
            around = refs[-2:]
            del refs[-2:]
            targets += around
            del refs[:1]
        else:
            del refs[:2]
    out, heat = refs[:2]
    window, even, odd, coef, kept, result, thick, warm = refs[2:10]
    in_sems, coef_sems, out_sems, heat_sems, once_sems = refs[10:]
    once = [
        pltpu.make_async_copy(x, y, once_sems.at[i])
        for i, (x, y) in enumerate(zip(sources, targets))
    ]

    columns = 8
    wide = columns + 2 * SUB
    mine, z = place[0], place[1]
    parity = lax.rem(mine, 2)
    blocks = out.shape[2] // LANES
    grid_rows = out.shape[2]
    top = MARGIN + LANES

    sublane = lax.broadcasted_iota(jnp.int32, (8, LANES), 0)
    weights = jnp.zeros((8, LANES), jnp.float32)
    for w in range(NW):
        weights = jnp.where(sublane == NW + w, sunlight[w], weights)

    def wide_of(x):
        return x.astype(jnp.float32)

    def loads(j, slot, level):
        block = lax.rem(mine + 1 + sum(CHUNKS[:k]) + j, blocks)
        row = pl.multiple_of(block * LANES, LANES)
        low = pl.multiple_of(jnp.maximum(row - MARGIN, 0), MARGIN)
        high = pl.multiple_of(jnp.minimum(row + LANES, grid_rows - MARGIN), MARGIN)
        return [
            pltpu.make_async_copy(
                tracer.at[level, :, pl.ds(at, n), :],
                window.at[slot, level, :, to : to + n, :],
                in_sems.at[slot, level, i],
            )
            for i, (at, to, n) in enumerate(
                ((low, 0, MARGIN), (row, MARGIN, LANES), (high, MARGIN + LANES, MARGIN))
            )
        ]

    def load_block(j, slot):
        for level in (1, 0):
            for copy in loads(j, slot, level):
                copy.start()

    def coef_loads(j, level):
        block = lax.rem(mine + 1 + sum(CHUNKS[:k]) + j, blocks)
        these = [
            pltpu.make_async_copy(all_coef.at[block, level], coef.at[level], coef_sems.at[level])
        ]
        if level == 0:
            these.append(pltpu.make_async_copy(all_share.at[block], kept, coef_sems.at[2]))
        return these

    def copies(j, slot, which=None):
        block = lax.rem(mine + 1 + sum(CHUNKS[:k]) + j, blocks)
        row = pl.multiple_of(block * LANES, LANES)
        these = []
        for level in (0, 1) if which is None else (which,):
            if level < 2:
                source, target = result.at[slot, level], out.at[level, :, pl.ds(row, LANES), :]
                these.append(pltpu.make_async_copy(source, target, out_sems.at[slot, level]))
        if which == 2 or (which is None and not final):
            these.append(pltpu.make_async_copy(warm.at[slot], heat.at[block], heat_sems.at[slot]))
        return these

    def field_row(block, at):
        return fields[block, at : at + 1, :]

    def step(level, source, c, i, r0, n):
        here = source[c, r0 : r0 + n, :]
        u = coef[level, 2 * i, r0 - NEAR : r0 - NEAR + n, :]
        v = coef[level, 2 * i + 1, r0 - NEAR : r0 - NEAR + n, :]
        across = jnp.where(u > 0.0, source[c - 1, r0 : r0 + n, :], source[c + 1, r0 : r0 + n, :])
        along = jnp.where(
            v > 0.0, source[c, pl.ds(z + (r0 - 1), n), :], source[c, pl.ds(z + (r0 + 1), n), :]
        )
        return here - jnp.abs(u) * (here - across) - jnp.abs(v) * (here - along)

    def one_block(j, carry):
        slot = lax.rem(j, 2)
        block = lax.rem(mine + 1 + sum(CHUNKS[:k]) + j, blocks)
        has_low = jnp.where(block != 0, 1.0, 0.0)
        has_high = jnp.where(block != blocks - 1, 1.0, 0.0)

        if count > 1:

            @pl.when(j + 1 < count)
            def _():
                load_block(j + 1, 1 - slot)

        if count > 2:

            @pl.when(j >= 2)
            def _():
                for copy in copies(j - 2, slot):
                    copy.wait()

        for level in (1, 0):
            def widen(at, low, head, tail, high):
                even[at, NEAR:MARGIN, :] = wide_of(low)[NEAR:, :] * has_low
                even[at, MARGIN : 2 * MARGIN, :] = wide_of(head)
                even[at, 2 * MARGIN : top, :] = wide_of(tail)
                even[at, top : top + NEAR, :] = wide_of(high)[:NEAR, :] * has_high

            for copy in loads(j, slot, level):
                copy.wait()

            def widen_column(x, carry):
                parts = [
                    window[slot, level, x, r : r + n, :]
                    for r, n in (
                        (0, MARGIN),
                        (MARGIN, MARGIN),
                        (2 * MARGIN, LANES - MARGIN),
                        (top, MARGIN),
                    )
                ]
                widen(SUB + x, *parts)
                return carry

            lax.fori_loop(0, columns, widen_column, 0)

            def rims(at_start):
                for swap, (rim, prior) in enumerate(zip(halos, before)):
                    for c in range(SUB):
                        at = c + (parity if swap else 1 - parity) * (SUB + columns)
                        if at_start:
                            low = prior[level, c, 0:MARGIN, :]
                            head = prior[level, c, MARGIN : 2 * MARGIN, :]
                            tail = rim[level, c, 0 : LANES - MARGIN, :]
                            if final:
                                high = around[swap][level, c]
                            else:
                                high = rim[level, c, LANES - MARGIN : LANES, :]
                        else:
                            base = j * LANES + (0 if first else -2 * MARGIN)
                            low, head, tail, high = (
                                rim[level, c, pl.ds(pl.multiple_of(base + a, MARGIN), n), :]
                                for a, n in (
                                    (0, MARGIN),
                                    (MARGIN, MARGIN),
                                    (2 * MARGIN, LANES - MARGIN),
                                    (top, MARGIN),
                                )
                            )
                        widen(at, low, head, tail, high)

            if level == 1:

                def once_wait():
                    for copy in once:
                        copy.wait()

                if count == 1:
                    once_wait()
                else:
                    pl.when(j == 0)(once_wait)

            if first:
                rims(False)
            elif count == 1:
                rims(True)
            else:
                pl.when(j == 0)(functools.partial(rims, True))
                pl.when(j != 0)(functools.partial(rims, False))

            def substep_one(c, carry):
                for r0, n in row_blocks(NEAR, LANES + 2 * NEAR, 72):
                    odd[c, r0 : r0 + n, :] = step(level, even, c, c - 1, r0, n)
                return carry

            def substep_two(c, carry):
                for r0, n in row_blocks(NEAR, LANES + 2 * NEAR, 72):
                    even[c, r0 : r0 + n, :] = step(level, odd, c, c - 1, r0, n)
                return carry

            for copy in coef_loads(j, level):
                copy.wait()
            if level == 1:

                def load_rest():
                    for copy in coef_loads(0, 0):
                        copy.start()

                if count == 1:
                    load_rest()
                else:
                    pl.when(j == 0)(load_rest)
            lax.fori_loop(1, wide - 1, substep_one, 0, unroll=4)
            lax.fori_loop(2, wide - 2, substep_two, 0, unroll=5)

            def substep_three(x, carry):
                c = x + SUB
                for r0, n in row_blocks(MARGIN, LANES, 64):
                    now = step(level, even, c, c - 1, r0, n)
                    if level == 0:
                        now = now * kept[x, r0 - MARGIN : r0 - MARGIN + n, :]
                    result[slot, level, x, r0 - MARGIN : r0 - MARGIN + n, :] = now
                return carry

            lax.fori_loop(0, columns, substep_three, 0, unroll=4)
            copies(j, slot, level)[0].start()
            if count > 1:

                @pl.when(j + 1 < count)
                def _():
                    for copy in coef_loads(j + 1, level):
                        copy.start()

            for x in range(columns):
                rounded = result[slot, level, x].astype(jnp.bfloat16)
                projected = lax.dot_general(
                    table[...], rounded, (((1,), (1,)), ((), ())), preferred_element_type=jnp.float32
                )
                which = classes[block, x : x + 1, :]
                dry = jnp.zeros((8, LANES), jnp.float32)
                wet = jnp.zeros((8, LANES), jnp.float32)
                for b in range(NBIN):
                    dry = jnp.where(which == b, projected[8 * b : 8 * b + 8], dry)
                    wet = jnp.where(which == b, projected[64 + 8 * b : 72 + 8 * b], wet)
                at = 8 * level + x
                moist = field_row(block, MOIST_ROW + at)
                thickness = field_row(block, DEPTH_ROW + at)
                sun = field_row(block, SUN_ROW + x)
                growth = moist / (1.0 - moist)
                optical = (dry + growth * wet) * thickness
                if level == 1:
                    thick[x] = optical
                    lit = weights * optical
                else:
                    overhead = pltpu.roll(thick[x], NW, 0)
                    lit = weights * optical * jnp.exp(-overhead / sun)
                lit = sun * jnp.sum(lit, axis=0, keepdims=True)
                if final:
                    heat[at : at + 1, :] = lit
                else:
                    warm[slot, at : at + 1, :] = lit
        if not final:
            copies(j, slot, 2)[0].start()
        return carry

    for copy in coef_loads(0, 1):
        copy.start()
    load_block(0, 0)
    for copy in once:
        copy.start()
    if count == 1:
        one_block(0, 0)
    else:
        lax.fori_loop(0, count, one_block, 0)
    for j in range(max(count - 2, 0), count):
        for copy in copies(j, j % 2):
            copy.wait()
    if first:
        copy = pltpu.make_async_copy(warm.at[0], heat.at[mine], heat_sems.at[0])
        copy.start()
        copy.wait()


def chunk_call(k, operands, out, heat, shape, gy):
    first, final = k == 0, k == len(CHUNKS) - 1
    levels, columns, _, _ = shape
    vmem = pl.BlockSpec(memory_space=pltpu.VMEM)
    smem = pl.BlockSpec(memory_space=pltpu.SMEM)
    hbm = pl.BlockSpec(memory_space=pltpu.HBM)
    operands = list(operands)
    specs = [smem, smem] + [hbm] * (len(operands) - 2)
    heat_block = (levels * columns, LANES)
    out_shapes = [jax.ShapeDtypeStruct(shape, jnp.float32)]
    out_specs = [hbm]
    aliases = {}
    if not first:
        aliases[len(operands)] = 0
        operands.append(out)
        specs.append(hbm)
    if final:
        out_shapes.append(jax.ShapeDtypeStruct(heat_block, jnp.float32))
        out_specs.append(vmem)
    else:
        if not first:
            aliases[len(operands)] = 1
            operands.append(heat)
            specs.append(hbm)
        out_shapes.append(jax.ShapeDtypeStruct((gy,) + heat_block, jnp.float32))
        out_specs.append(hbm)
    table, fields, classes = operands[2:5]
    rim = (levels, SUB, 2 * MARGIN, LANES)
    kept = [pltpu.VMEM((levels, SUB, MARGIN, LANES), jnp.bfloat16)] * (2 * final)
    kept += [pltpu.VMEM(rim, jnp.bfloat16)] * (2 * (not first))
    kept += [pltpu.VMEM(x.shape, x.dtype) for x in operands[8:10] + [table, fields, classes]]
    work = CHUNKS[k] * LANES * columns * levels * LANES
    return pl.pallas_call(
        functools.partial(chunk_kernel, k),
        out_shape=tuple(out_shapes),
        in_specs=specs,
        out_specs=tuple(out_specs),
        scratch_shapes=[
            pltpu.VMEM((2, levels, columns, SPAN, LANES), jnp.bfloat16),
            pltpu.VMEM((columns + 2 * SUB, SPAN, LANES), jnp.float32),
            pltpu.VMEM((columns + 2 * SUB, SPAN, LANES), jnp.float32),
            pltpu.VMEM((levels, 24, COEF_SPAN, LANES), jnp.float32),
            pltpu.VMEM((columns, LANES, LANES), jnp.float32),
            pltpu.VMEM((2, levels, columns, LANES, LANES), jnp.float32),
            pltpu.VMEM((columns, 8, LANES), jnp.float32),
            pltpu.VMEM((2, levels * columns, LANES), jnp.float32),
            pltpu.SemaphoreType.DMA((2, levels, 3)),
            pltpu.SemaphoreType.DMA((3,)),
            pltpu.SemaphoreType.DMA((2, levels)),
            pltpu.SemaphoreType.DMA((2,)),
            pltpu.SemaphoreType.DMA((len(kept),)),
            *kept,
        ],
        input_output_aliases=aliases,
        compiler_params=pltpu.CompilerParams(vmem_limit_bytes=16 * 1024 * 1024),
        cost_estimate=pl.CostEstimate(flops=60 * work, transcendentals=0, bytes_accessed=8 * work),
    )(*operands)


def per_device(
    tracer_amounts,
    zonal_transit_ratio,
    meridional_transit_ratio,
    moisture_ratio,
    stratum_depths,
    sun_elevation_factor,
    thermal_anomaly,
    particle_class_map,
    ground_cover_kind,
    arid_extinction_table,
    swelling_factors,
    settling_velocities,
    arriving_irradiance,
):
    f32, bf16 = jnp.float32, jnp.bfloat16
    levels, columns, _, species = tracer_amounts.shape
    tile = thermal_anomaly.shape[1]
    gx, gy = lax.axis_size("gx"), lax.axis_size("gy")
    strips = ("gx", "gy")

    def swaps(n):
        pairs = [[(i, i + 1) for i in range(start, n - 1, 2)] for start in (0, 1)]
        return [p + [(j, i) for i, j in p] for p in pairs]

    vmem = pl.BlockSpec(memory_space=pltpu.VMEM)
    smem = pl.BlockSpec(memory_space=pltpu.SMEM)
    hbm = pl.BlockSpec(memory_space=pltpu.HBM)

    mine = lax.axis_index("gy").astype(jnp.int32)
    gx_odd = lax.rem(lax.axis_index("gx").astype(jnp.int32), 2)
    place = jnp.stack([mine, jnp.zeros((), jnp.int32), gx_odd])

    def halo_shape(k):
        low, high = chunk_rows(k)
        return jax.ShapeDtypeStruct((levels, SUB, high - low, species), bf16)

    rim_shape = jax.ShapeDtypeStruct((2 * 8, LANES), f32)
    *slices, rim_0, rim_1 = pl.pallas_call(
        first_slice_kernel,
        out_shape=(halo_shape(0), halo_shape(0), rim_shape, rim_shape),
        in_specs=[smem, hbm] + [vmem] * 3,
        out_specs=(vmem,) * 4,
        scratch_shapes=[pltpu.SemaphoreType.DMA((copy_count((0,)),))],
        compiler_params=pltpu.CompilerParams(vmem_limit_bytes=4 * 1024 * 1024),
        name="slice_first",
    )(
        place,
        *hold(tracer_amounts, zonal_transit_ratio, meridional_transit_ratio, thermal_anomaly),
    )
    later = tuple(range(1, len(CHUNKS)))
    later_shapes = [halo_shape(k) for k in later for _ in range(2)]
    slices += hold(
        *pl.pallas_call(
            later_slice_kernel,
            out_shape=tuple(pltpu.HBM(x.shape, x.dtype) for x in later_shapes),
            in_specs=[smem, hbm],
            out_specs=(hbm,) * len(later_shapes),
            scratch_shapes=[pltpu.VMEM(x.shape, x.dtype) for x in later_shapes]
            + [
                pltpu.SemaphoreType.DMA((copy_count(later),)),
                pltpu.SemaphoreType.DMA((len(later_shapes),)),
            ],
            compiler_params=pltpu.CompilerParams(vmem_limit_bytes=8 * 1024 * 1024),
            name="slice_later",
        )(place, *hold(tracer_amounts))
    )

    rims = [lax.ppermute(r, "gx", p) for r, p in zip((rim_0, rim_1), swaps(gx))]
    halos = []
    for k in range(len(CHUNKS)):
        pair = slices[2 * k : 2 * k + 2]
        halos.append([lax.ppermute(h, strips, p) for h, p in zip(pair, swaps(gx * gy))])

    packed = pl.pallas_call(
        pack_kernel,
        out_shape=jax.ShapeDtypeStruct((gy, FIELD_ROWS, LANES), f32),
        in_specs=[smem] + [vmem] * 8,
        out_specs=vmem,
        scratch_shapes=[pltpu.VMEM((4, tile + 16, LANES), f32)],
        compiler_params=pltpu.CompilerParams(vmem_limit_bytes=4 * 1024 * 1024),
        name="pack",
    )(
        place,
        *hold(
            zonal_transit_ratio,
            meridional_transit_ratio,
            moisture_ratio,
            stratum_depths,
            sun_elevation_factor,
            thermal_anomaly,
        ),
        *rims,
    )
    fields = lax.all_to_all(packed, "gy", split_axis=0, concat_axis=0, tiled=True)

    turned, classes = pl.pallas_call(
        turn_kernel,
        out_shape=(
            jax.ShapeDtypeStruct((levels, gy, LANES, LANES), bf16),
            jax.ShapeDtypeStruct((gy, columns, LANES), jnp.int32),
        ),
        in_specs=[vmem] * 3,
        out_specs=(vmem, vmem),
        compiler_params=pltpu.CompilerParams(vmem_limit_bytes=4 * 1024 * 1024),
        name="turn",
    )(fields, *hold(ground_cover_kind, particle_class_map))

    warmed = pl.pallas_call(
        warm_kernel,
        out_shape=jax.ShapeDtypeStruct(thermal_anomaly.shape, f32),
        in_specs=[smem] + [vmem] * 4,
        out_specs=vmem,
        scratch_shapes=[pltpu.VMEM((tile + 16, LANES), f32)],
        compiler_params=pltpu.CompilerParams(vmem_limit_bytes=4 * 1024 * 1024),
        name="warm",
    )(place, *hold(thermal_anomaly), *rims, fields)

    spread = jnp.asarray(spread_matrix(), bf16)
    table = jnp.concatenate([arid_extinction_table, swelling_factors], axis=1).T
    parts, rest = [], settling_velocities
    for _ in range(3):
        part = lax.reduce_precision(rest, 8, 7)
        parts.append(part.astype(bf16))
        rest = rest - part
    parts.append(jnp.zeros((LANES - 3 * settling_velocities.shape[0], species), bf16))
    speeds = jnp.concatenate(parts, axis=0)

    coef_shape = (24, LANES + 2 * NEAR, LANES)
    coefficients = pl.pallas_call(
        coefficient_kernel,
        out_shape=(
            pltpu.HBM((gy, levels) + coef_shape, f32),
            pltpu.HBM((gy, columns, LANES, LANES), f32),
        ),
        in_specs=[vmem] * 3,
        out_specs=(hbm, hbm),
        scratch_shapes=[
            pltpu.VMEM((levels,) + coef_shape, f32),
            pltpu.VMEM((columns, LANES, LANES), bf16),
            pltpu.VMEM((columns, LANES, LANES), f32),
            pltpu.SemaphoreType.DMA((levels,)),
            pltpu.SemaphoreType.DMA((1,)),
        ],
        compiler_params=pltpu.CompilerParams(vmem_limit_bytes=12 * 1024 * 1024),
        name="coefficients",
    )(turned, spread, speeds)

    def run_chunk(k, out, heat):
        operands = [table, fields, classes]
        final = k == len(CHUNKS) - 1
        for n in [k] + [k - 1] * (k > 0) + [0] * final:
            operands += halos[n]
        own = halos[k]
        operands = hold(*operands[:3]) + own + hold(*operands[5:])
        held = hold(tracer_amounts, *coefficients)
        operands = [place, arriving_irradiance] + operands[:3] + held + operands[3:]
        return chunk_call(k, operands, out, heat, tracer_amounts.shape, gy)

    out = heat = None
    for k in range(len(CHUNKS) - 1):
        out, heat = run_chunk(k, out, heat)
    returned = lax.all_to_all(heat, "gy", split_axis=0, concat_axis=0, tiled=True)
    out, own = run_chunk(len(CHUNKS) - 1, out, None)

    is_own = lax.broadcasted_iota(jnp.int32, (gy, 1, 1), 0) == mine
    returned = jnp.where(is_own, own[None], returned)
    returned = returned.reshape(gy, levels, columns, LANES).transpose(1, 0, 2, 3)
    return out, warmed + returned.reshape(thermal_anomaly.shape)


def solution(mesh):
    return jax.shard_map(
        per_device,
        mesh=mesh,
        in_specs=(
            P(None, ("gx", "gy"), None, None),
            P(None, "gx", "gy"),
            P(None, "gx", "gy"),
            P(None, "gx", "gy"),
            P(None, "gx", "gy"),
            P("gx", "gy"),
            P(None, "gx", "gy"),
            P(("gx", "gy"), None),
            P(("gx", "gy"), None),
            P(),
            P(),
            P(),
            P(),
        ),
        out_specs=(P(None, ("gx", "gy"), None, None), P(None, "gx", "gy")),
        check_vma=False,
    )
```
